16 devices in a mesh: sp: 16 (over z, y, x, core).
Axes of the slice: x: 2, y: 2, z: 2, core: 2. Of those that a mesh axis runs over, the one named last changes fastest.
Arguments:
- x_in: bfloat16 [2, 2048, 3072], P(None, 'sp')
- grad_y: bfloat16 [2, 2048, 3072], P(None, 'sp')
- ln_gain: float32 [3072], replicated
- ln_bias: float32 [3072], replicated
- w_qkv: bfloat16 [3072, 3, 32, 96], replicated
- b_qkv: float32 [3, 32, 96], replicated
- w_out: bfloat16 [32, 96, 3072], replicated
- b_out: float32 [3072], replicated
Outputs:
- output 1: bfloat16 [2, 2048, 3072], P(None, 'sp')
- output 2: bfloat16 [2, 2048, 3072], P(None, 'sp')
- output 3: float32 [3072], replicated
- output 4: float32 [3072], replicated
- output 5: float32 [3072, 3, 32, 96], replicated
- output 6: float32 [3, 32, 96], replicated
- output 7: float32 [32, 96, 3072], replicated
- output 8: float32 [3072], replicated
All inputs are finite; a program needn't handle non-finite values.
Results may differ from the reference program's by a relative error of at most 0.0138752.
Values are sent between devices in bfloat16 or wider.
A program may use at most 1 GiB of HBM per device.

```python
import jax
import jax.numpy as jnp
from jax import lax

BATCH_SIZE = 2
SEQ_LEN = 2048
MODEL_DIM = 3072
NUM_HEADS = 32
HEAD_DIM = 96

LN_EPS = 1e-5
ATTN_SCALE = HEAD_DIM ** -0.5


def setup_inputs(seed: int = 0) -> dict:
    keys_all = jax.random.split(jax.random.key(seed), 8)
    act_shape = (BATCH_SIZE, SEQ_LEN, MODEL_DIM)
    x_in = jax.random.normal(keys_all[0], act_shape, jnp.float32).astype(jnp.bfloat16)
    grad_y = jax.random.normal(keys_all[1], act_shape, jnp.float32).astype(jnp.bfloat16)
    ln_gain = 1.4 + 0.3 * jax.random.normal(keys_all[2], (MODEL_DIM,), jnp.float32)
    ln_bias = 0.3 * jax.random.normal(keys_all[3], (MODEL_DIM,), jnp.float32)
    w_qkv = (jax.random.normal(keys_all[4], (MODEL_DIM, 3, NUM_HEADS, HEAD_DIM), jnp.float32) * MODEL_DIM ** -0.5).astype(jnp.bfloat16)
    b_qkv = 0.5 * jax.random.normal(keys_all[5], (3, NUM_HEADS, HEAD_DIM), jnp.float32)
    w_out = (jax.random.normal(keys_all[6], (NUM_HEADS, HEAD_DIM, MODEL_DIM), jnp.float32) * (NUM_HEADS * HEAD_DIM) ** -0.5).astype(jnp.bfloat16)
    b_out = 0.5 * jax.random.normal(keys_all[7], (MODEL_DIM,), jnp.float32)
    return {"x_in": x_in, "grad_y": grad_y, "ln_gain": ln_gain, "ln_bias": ln_bias, "w_qkv": w_qkv, "b_qkv": b_qkv, "w_out": w_out, "b_out": b_out}


def head_attention(qkv_head):
    q_head = qkv_head[0].astype(jnp.float32)
    k_head = qkv_head[1].astype(jnp.float32)
    v_head = qkv_head[2].astype(jnp.float32)
    scores = jnp.einsum("bqe,bke->bqk", q_head, k_head) * ATTN_SCALE
    positions = jnp.arange(SEQ_LEN)
    causal = positions[:, None] >= positions[None, :]
    scores = jnp.where(causal, scores, -1e30)
    prob_low = jax.nn.softmax(scores, axis=-1).astype(jnp.bfloat16).astype(jnp.float32)
    return jnp.einsum("bqk,bke->bqe", prob_low, v_head).astype(jnp.bfloat16)


def block_forward(x_in, ln_gain, ln_bias, w_qkv, b_qkv, w_out, b_out):
    x_float = x_in.astype(jnp.float32)
    centered = x_float - jnp.mean(x_float, axis=-1, keepdims=True)
    variance = jnp.mean(centered * centered, axis=-1, keepdims=True)
    normed = (centered * lax.rsqrt(variance + LN_EPS) * ln_gain + ln_bias).astype(jnp.bfloat16)
    flat_tokens = normed.reshape(BATCH_SIZE * SEQ_LEN, MODEL_DIM).astype(jnp.float32)
    qkv_proj = jnp.dot(flat_tokens, w_qkv.reshape(MODEL_DIM, 3 * NUM_HEADS * HEAD_DIM), preferred_element_type=jnp.float32)
    qkv_proj = (qkv_proj.reshape(BATCH_SIZE, SEQ_LEN, 3, NUM_HEADS, HEAD_DIM) + b_qkv).astype(jnp.bfloat16)
    head_major = jnp.transpose(qkv_proj, (3, 2, 0, 1, 4))
    attn_heads = lax.map(jax.checkpoint(head_attention), head_major)
    attn_flat = jnp.transpose(attn_heads, (1, 2, 0, 3)).reshape(BATCH_SIZE * SEQ_LEN, NUM_HEADS * HEAD_DIM)
    proj_out = jnp.dot(attn_flat.astype(jnp.float32), w_out.reshape(NUM_HEADS * HEAD_DIM, MODEL_DIM), preferred_element_type=jnp.float32) + b_out
    return (x_float + proj_out.reshape(BATCH_SIZE, SEQ_LEN, MODEL_DIM)).astype(jnp.bfloat16)


def reference(x_in, grad_y, ln_gain, ln_bias, w_qkv, b_qkv, w_out, b_out):
    y_out, pullback = jax.vjp(block_forward, x_in, ln_gain, ln_bias, w_qkv.astype(jnp.float32), b_qkv, w_out.astype(jnp.float32), b_out)
    all_grads = pullback(grad_y)
    return (y_out, all_grads[0], all_grads[1], all_grads[2], all_grads[3], all_grads[4], all_grads[5], all_grads[6])
```

```python
import functools
import math

import jax
import jax.numpy as jnp
from jax import lax
from jax.experimental import pallas as pl
from jax.experimental.pallas import tpu as pltpu
from jax.sharding import PartitionSpec as P


LN_EPS = 1e-5
F32 = jnp.float32
BF16 = jnp.bfloat16
VMEM_LIMIT = 64 * 1024 * 1024 - 65536

B, S, D, NH, DH = 2, 2048, 3072, 32, 96
NDEV = 16
TOK = S // NDEV
GH = 4
GR = GH * DH
CR = 4 * GR
SCALE = DH ** -0.5
BQ = 512


def dot_nt(a, b):
    return lax.dot_general(a, b, (((1,), (1,)), ((), ())), preferred_element_type=F32)


def dot_nn(a, b):
    return jnp.dot(a, b, preferred_element_type=F32)


def params(**kw):
    return pltpu.CompilerParams(vmem_limit_bytes=VMEM_LIMIT, **kw)


def proj_kernel(wt_ref, wo_ref, bias_ref, s_ref, qkv_ref, do_ref):
    u = jnp.concatenate([s_ref[0, :TOK], s_ref[1, :TOK]], axis=0)
    gy = jnp.concatenate([s_ref[0, TOK:], s_ref[1, TOK:]], axis=0)
    qkv_ref[...] = (dot_nt(wt_ref[...], u) + bias_ref[...]).astype(BF16)
    do_ref[...] = dot_nt(wo_ref[...], gy).astype(BF16)


def project(wt, wo, bias, gathered):
    full = lambda i: (0, 0)
    return pl.pallas_call(
        proj_kernel,
        grid=(NDEV // 2,),
        in_specs=[
            pl.BlockSpec((3 * GR, D), full),
            pl.BlockSpec((GR, D), full),
            pl.BlockSpec((3 * GR, 1), full),
            pl.BlockSpec((2, 2 * TOK, D), lambda i: (i, 0, 0)),
        ],
        out_specs=[
            pl.BlockSpec((3 * GR, 2 * TOK), lambda i: (0, i)),
            pl.BlockSpec((GR, 2 * TOK), lambda i: (0, i)),
        ],
        out_shape=[jax.ShapeDtypeStruct((3 * GR, S), BF16), jax.ShapeDtypeStruct((GR, S), BF16)],
        compiler_params=params(),
        cost_estimate=pl.CostEstimate(flops=2 * 4 * GR * D * S, bytes_accessed=35_000_000, transcendentals=0),
        name="project",
    )(wt, wo, bias, gathered)


def att_kernel(q_ref, k_ref, v_ref, do_ref, o_ref, dq_ref, dk_ref, dv_ref, db_ref, dk_acc, dv_acc):
    to_exp2 = SCALE * math.log2(math.e)
    k_t = k_ref[...]
    v_t = v_ref[...]
    k_n = k_t.T
    v_n = v_t.T
    db_q = jnp.zeros((DH, 1), F32)
    for i in reversed(range(S // BQ)):
        keys = (i + 1) * BQ
        cols = slice(i * BQ, keys)
        q = q_ref[:, cols]
        do = do_ref[:, cols]
        s = dot_nn(k_n[:keys], q)
        row = lax.broadcasted_iota(jnp.int32, (BQ, BQ), 0)
        col = lax.broadcasted_iota(jnp.int32, (BQ, BQ), 1)
        s_diag = jnp.where(row <= col, s[keys - BQ:], -1e30)
        s = jnp.concatenate([s[:keys - BQ], s_diag], axis=0) if i else s_diag
        m = jnp.max(s, axis=0, keepdims=True)
        p = jnp.exp2((s - m) * to_exp2)
        p = p * (1.0 / jnp.sum(p, axis=0, keepdims=True))
        p_low = p.astype(BF16)
        o_ref[:, cols] = dot_nn(v_t[:, :keys], p_low).astype(BF16)
        dp = dot_nn(v_n[:keys], do).astype(BF16).astype(F32)
        row_dot = jnp.sum(p * dp, axis=0, keepdims=True)
        ds = (p * (dp - row_dot) * SCALE).astype(BF16)
        dq = dot_nn(k_t[:, :keys], ds).astype(BF16)
        dq_ref[:, cols] = dq
        db_q += jnp.sum(dq.astype(F32), axis=1, keepdims=True)
        dk = dot_nt(q, ds)
        dv = dot_nt(do, p_low)
        if keys == S:
            dk_acc[...] = dk
            dv_acc[...] = dv
        else:
            dk_acc[:, :keys] += dk
            dv_acc[:, :keys] += dv
    dk = dk_acc[...].astype(BF16)
    dv = dv_acc[...].astype(BF16)
    dk_ref[...] = dk
    dv_ref[...] = dv
    db_k = jnp.sum(dk.astype(F32), axis=1, keepdims=True)
    db_v = jnp.sum(dv.astype(F32), axis=1, keepdims=True)
    for t, db in enumerate((db_q, db_k, db_v)):
        db_ref[t] = jnp.broadcast_to(db, (DH, 128))


def attention(qkv, do):
    spec = lambda off: pl.BlockSpec((DH, S), lambda h: (h + off, 0))
    return pl.pallas_call(
        att_kernel,
        grid=(GH,),
        in_specs=[spec(0), spec(GH), spec(2 * GH), spec(0)],
        out_specs=[spec(0)] * 4 + [pl.BlockSpec((3, DH, 128), lambda h: (0, h, 0))],
        out_shape=[jax.ShapeDtypeStruct((GR, S), BF16)] * 4 + [jax.ShapeDtypeStruct((3, GR, 128), F32)],
        scratch_shapes=[pltpu.VMEM((DH, S), F32)] * 2,
        compiler_params=params(),
        cost_estimate=pl.CostEstimate(flops=40_000_000_000, bytes_accessed=12_000_000, transcendentals=0),
        name="attention",
    )(qkv, qkv, qkv, do)


def collect_kernel(tbl, *refs):
    own_ref, peer_ref = refs[16:]
    for s in range(4):
        rows = pl.ds(pl.multiple_of(tbl[3 + s] * GR, GR), GR)
        for b in range(2):
            own_ref[rows, b * TOK:(b + 1) * TOK] = refs[s * 2 + b][...]
            peer_ref[rows, b * TOK:(b + 1) * TOK] = refs[8 + s * 2 + b][...]


def collect(tbl, pieces):
    own = pl.BlockSpec((GR, TOK), lambda i, t: (0, t[1]))
    peer = pl.BlockSpec((GR, TOK), lambda i, t: (0, t[2]))
    whole = pl.BlockSpec((CR, 2 * TOK), lambda i, t: (0, 0))
    return pl.pallas_call(
        collect_kernel,
        grid_spec=pltpu.PrefetchScalarGridSpec(
            num_scalar_prefetch=1, grid=(1,), in_specs=[own] * 8 + [peer] * 8, out_specs=[whole] * 2),
        out_shape=[jax.ShapeDtypeStruct((CR, 2 * TOK), BF16)] * 2,
        compiler_params=params(),
        cost_estimate=pl.CostEstimate(flops=1_000_000_000, bytes_accessed=3_000_000, transcendentals=0),
        name="collect",
    )(tbl, *pieces, *pieces)


BD = 256


def dw_kernel(tbl, x0, x1, *refs):
    pieces = refs[:8]
    out_ref, ex_ref, lhs_ref, sem = refs[-4:]

    @pl.when(pl.program_id(0) == 0)
    def _():
        copies = []
        for s in range(4):
            rows = pl.ds(pl.multiple_of(tbl[3 + s] * GR, GR), GR)
            for b in range(B):
                copies.append(pltpu.make_async_copy(
                    pieces[2 * s + b], lhs_ref.at[rows, pl.ds(b * S, S)], sem.at[2 * s + b]))
        for c in copies:
            c.start()
        for c in copies:
            c.wait()

    x = jnp.concatenate([x0[r] for r in range(NDEV)] + [x1[r] for r in range(NDEV)], axis=0)
    res = dot_nn(lhs_ref[...], x)
    out_ref[...] = res
    ex_ref[...] = res


def weight_grad(tbl, gathered, pieces, row_block, which, out_rows, prev=None):
    x_spec = pl.BlockSpec((NDEV, TOK, BD), lambda j, t: (0, which, j))
    anywhere = pl.BlockSpec(memory_space=pl.ANY)
    in_specs = [x_spec] * 2 + [anywhere] * 8
    args = [tbl, *gathered, *pieces]
    alias = {}
    if prev is not None:
        in_specs.append(anywhere)
        args.append(prev)
        alias = {len(args) - 1: 0}
    return pl.pallas_call(
        dw_kernel,
        grid_spec=pltpu.PrefetchScalarGridSpec(
            num_scalar_prefetch=1,
            grid=(D // BD,),
            in_specs=in_specs,
            out_specs=[
                pl.BlockSpec((CR, BD), lambda j, t: (2 * row_block + t[0], j)),
                pl.BlockSpec((CR, BD), lambda j, t: (0, j)),
            ],
            scratch_shapes=[pltpu.VMEM((CR, B * S), BF16), pltpu.SemaphoreType.DMA((8,))]),
        out_shape=[jax.ShapeDtypeStruct((out_rows, D), F32), jax.ShapeDtypeStruct((CR, D), F32)],
        input_output_aliases=alias,
        compiler_params=params(),
        cost_estimate=pl.CostEstimate(flops=2 * CR * D * B * S, bytes_accessed=75_000_000, transcendentals=0),
        name="weight_grad",
    )(*args)


def contract_kernel(first, tbl, here_ref, there_ref, w_ref, *refs):
    acc_ref = refs[-1]
    i = pl.program_id(0)

    @pl.when(i == 0)
    def _():
        acc_ref[...] = jnp.zeros_like(acc_ref) if first else refs[0][...]

    rows = pl.ds(pl.multiple_of((i % 4) * GR, GR), GR)
    act = jnp.where(i // 4 == tbl[0], here_ref[rows, :], there_ref[rows, :])
    acc_ref[...] += lax.dot_general(act, w_ref[...], (((0,), (0,)), ((), ())), preferred_element_type=F32)


def contract(tbl, here, there, weight, block, acc=None):
    whole = lambda shape: pl.BlockSpec(shape, lambda i, t: (0, 0))
    args = [tbl, here, there, weight] + ([] if acc is None else [acc])
    return pl.pallas_call(
        functools.partial(contract_kernel, acc is None),
        grid_spec=pltpu.PrefetchScalarGridSpec(
            num_scalar_prefetch=1,
            grid=(D // GR,),
            in_specs=[whole((CR, B * TOK))] * 2 + [pl.BlockSpec((GR, D), lambda i, t: (block * 8 + i, 0))]
            + ([] if acc is None else [whole((B * TOK, D))]),
            out_specs=whole((B * TOK, D))),
        out_shape=jax.ShapeDtypeStruct((B * TOK, D), F32),
        compiler_params=params(),
        cost_estimate=pl.CostEstimate(flops=2 * B * TOK * D * D, bytes_accessed=22_000_000, transcendentals=0),
        name="contract",
    )(*args)


def solution(mesh):
    def permute(a, bit):
        return lax.ppermute(a, "sp", [(i, i ^ bit) for i in range(NDEV)])

    def block(x_in, grad_y, ln_gain, ln_bias, w_qkv, b_qkv, w_out, b_out):
        me = lax.axis_index("sp")
        core = me % 2
        chip = me // 2
        group = lambda c: jnp.where(c < 4, c, 7 - c)
        groups = [group(chip), group(chip ^ 1), group(chip ^ 2), group(chip ^ 4)]
        tbl = jnp.stack([core, me, me ^ 1] + groups + [core]).astype(jnp.int32)
        mine = 4 * core + groups[0]

        x_float = x_in.astype(F32)
        centered = x_float - jnp.mean(x_float, axis=-1, keepdims=True)
        inv_std = lax.rsqrt(jnp.mean(centered * centered, axis=-1, keepdims=True) + LN_EPS)
        x_hat = centered * inv_std
        normed = (x_hat * ln_gain + ln_bias).astype(BF16)
        grad_b_out = jnp.sum(grad_y, axis=(0, 1), dtype=F32)

        w_rows = jnp.transpose(w_qkv, (1, 2, 3, 0)).reshape(3, 8, GR, D)
        wt = lax.dynamic_slice_in_dim(w_rows, mine, 1, axis=1).reshape(3 * GR, D)
        wo = lax.dynamic_slice_in_dim(w_out.reshape(8, GR, D), mine, 1, axis=0).reshape(GR, D)
        bias = lax.dynamic_slice_in_dim(b_qkv.reshape(3, 8, GR), mine, 1, axis=1).reshape(3 * GR, 1)

        local = [jnp.concatenate([normed[b], grad_y[b]], axis=0) for b in range(B)]
        g0 = lax.all_gather(local[0], "sp")
        second, g0 = lax.optimization_barrier((local[1], g0))
        g1 = lax.all_gather(second, "sp")
        gathered = [g0, g1]

        own = []
        for b in range(B):
            heads = project(wt, wo, bias, gathered[b])
            own.append(attention(*heads))
        db = own[0][4] + own[1][4]
        pieces = {}
        for name, idx in (("o", 0), ("v", 3), ("k", 2), ("q", 1)):
            got = []
            for s, bit in enumerate((0, 2, 4, 8)):
                for b in range(B):
                    got.append(own[b][idx] if s == 0 else permute(own[b][idx], bit))
            pieces[name] = got

        def tokens_of_mine(name, weight, block, acc=None):
            here, there = collect(tbl, pieces[name])
            there = permute(there, 1)
            return contract(tbl, here, there, weight, block, acc)

        proj_out = tokens_of_mine("o", w_out.reshape(D, D), 0).reshape(B, TOK, D) + b_out
        y_out = (x_float + proj_out).astype(BF16)

        def grad(name, t, prev=None):
            if name == "o":
                return weight_grad(tbl, gathered, pieces[name], 0, 1, D)
            return weight_grad(tbl, gathered, pieces[name], t, 0, 3 * D, prev)

        def put(buf, ex, t):
            ex = permute(ex, 1)
            return lax.dynamic_update_slice(buf, ex, (t * D + (1 - core) * CR, 0))

        gwo, ex_o = grad("o", 0)
        gwq, ex_v = grad("v", 2)
        gwq, ex_k = grad("k", 1, gwq)
        gwo = put(gwo, ex_o, 0)
        gwq = put(gwq, ex_v, 2)
        gwq, ex_q = grad("q", 0, gwq)
        gwq = put(gwq, ex_k, 1)
        gwq = put(gwq, ex_q, 0)

        flat_w = w_rows.reshape(3 * D, D)
        grad_normed = None
        for name, t in (("v", 2), ("k", 1), ("q", 0)):
            grad_normed = tokens_of_mine(name, flat_w, t, grad_normed)
        grad_normed = grad_normed.astype(BF16).astype(F32).reshape(B, TOK, D)
        grad_ln_gain = jnp.sum(grad_normed * x_hat, axis=(0, 1))
        grad_ln_bias = jnp.sum(grad_normed, axis=(0, 1))
        grad_hat = grad_normed * ln_gain
        mean_grad = jnp.mean(grad_hat, axis=-1, keepdims=True)
        mean_proj = jnp.mean(grad_hat * x_hat, axis=-1, keepdims=True)
        grad_x = (grad_y.astype(F32) + inv_std * (grad_hat - mean_grad - x_hat * mean_proj)).astype(BF16)

        db = jnp.where(chip < 4, db[:, :, 0], 0.0).reshape(3, 1, GR)
        db_all = lax.dynamic_update_slice(jnp.zeros((3, 8, GR), F32), db, (0, mine, 0)).reshape(3, D)
        small = jnp.concatenate([jnp.stack([grad_ln_gain, grad_ln_bias, grad_b_out]), db_all], axis=0)
        small = lax.psum(small, "sp")

        grad_w_qkv = jnp.transpose(gwq.reshape(3, NH, DH, D), (3, 0, 1, 2))
        return (y_out, grad_x, small[0], small[1], grad_w_qkv, small[3:6].reshape(3, NH, DH), gwo.reshape(NH, DH, D), small[2])

    seq = P(None, "sp", None)
    rep = P()

    return jax.shard_map(
        block, mesh=mesh, in_specs=(seq, seq, rep, rep, rep, rep, rep, rep),
        out_specs=(seq, seq, rep, rep, rep, rep, rep, rep), check_vma=False)
```

```python
import functools
import math

import jax
import jax.numpy as jnp
from jax import lax
from jax.experimental import pallas as pl
from jax.experimental.pallas import tpu as pltpu
from jax.sharding import PartitionSpec as P


LN_EPS = 1e-5
F32 = jnp.float32
BF16 = jnp.bfloat16
VMEM_LIMIT = 64 * 1024 * 1024 - 65536

B, S, D, NH, DH = 2, 2048, 3072, 32, 96
NDEV = 16
TOK = S // NDEV
GH = 4
GR = GH * DH
CR = 4 * GR
SCALE = DH ** -0.5
BQ = 512
LANES = 128


def dot_nt(a, b):
    return lax.dot_general(a, b, (((1,), (1,)), ((), ())), preferred_element_type=F32)


def dot_nn(a, b):
    return jnp.dot(a, b, preferred_element_type=F32)


def params(**kw):
    return pltpu.CompilerParams(vmem_limit_bytes=VMEM_LIMIT, **kw)


def cost(flops, moved):
    return pl.CostEstimate(flops=int(flops), bytes_accessed=int(moved), transcendentals=0)


ROWS = dict(axis=0, keepdims=True)
LAST_DIM = dict(axis=-1, keepdims=True)


def normalize(x):
    centered = x - jnp.mean(x, **LAST_DIM)
    inv_std = lax.rsqrt(jnp.mean(centered * centered, **LAST_DIM) + LN_EPS)
    return centered * inv_std, inv_std


def fixed(*shape):
    return pl.BlockSpec(shape, lambda *_: (0,) * len(shape))


def by_column(*shape):
    return pl.BlockSpec(shape, lambda j, *_: (0, j))


def aligned(start, size):
    return pl.ds(pl.multiple_of(start, size), size)


def run_all(copies, wait=False):
    for c in copies:
        c.wait() if wait else c.start()


dma = pltpu.SemaphoreType.DMA


def flip(index, bit):
    return index + bit * (1 - 2 * ((index // bit) % 2))


def att_head(q_ref, k_ref, v_ref, do_ref, o_ref, dq_ref, dk_ref, dv_ref, dk_acc, dv_acc):
    to_exp2 = SCALE * math.log2(math.e)
    k_t = k_ref[...]
    v_t = v_ref[...]
    k_n = k_t.T
    v_n = v_t.T
    db_q = jnp.zeros((DH, 1), F32)
    for i in reversed(range(S // BQ)):
        keys = (i + 1) * BQ
        cols = slice(i * BQ, keys)
        q = q_ref[:, cols]
        do = do_ref[:, cols]
        s = dot_nn(k_n[:keys], q)
        row = lax.broadcasted_iota(jnp.int32, (BQ, BQ), 0)
        col = lax.broadcasted_iota(jnp.int32, (BQ, BQ), 1)
        s_diag = jnp.where(row <= col, s[keys - BQ:], -1e30)
        s = jnp.concatenate([s[:keys - BQ], s_diag], axis=0) if i else s_diag
        m = jnp.max(s, **ROWS)
        p = jnp.exp2((s - m) * to_exp2)
        p = p * (1.0 / jnp.sum(p, **ROWS))
        p_low = p.astype(BF16)
        o = dot_nn(v_t[:, :keys], p_low)
        o_ref[:, cols] = o.astype(BF16)
        dp = dot_nn(v_n[:keys], do).astype(BF16).astype(F32)
        row_dot = jnp.sum(o * do.astype(F32), **ROWS)
        ds = (p * (dp - row_dot)).astype(BF16)
        dq = (dot_nn(k_t[:, :keys], ds) * SCALE).astype(BF16)
        dq_ref[:, cols] = dq
        db_q += jnp.sum(dq.astype(F32), **LAST_DIM)
        dk = dot_nt(q, ds)
        dv = dot_nt(do, p_low)
        if keys == S:
            dk_acc[...] = dk
            dv_acc[...] = dv
        else:
            dk_acc[:, :keys] += dk
            dv_acc[:, :keys] += dv
    dk = (dk_acc[...] * SCALE).astype(BF16)
    dv = dv_acc[...].astype(BF16)
    dk_ref[...] = dk
    dv_ref[...] = dv
    return db_q, jnp.sum(dk.astype(F32), **LAST_DIM), jnp.sum(dv.astype(F32), **LAST_DIM)


NEAR = (2, 4, 8)
VIA = {6: 4, 12: 8, 10: 2}
LAST = {12: 2, 10: 4, 6: 8}
SLOT = {d: i for i, d in enumerate((0, 2, 4, 8, 6, 12, 10, 14))}
N_SEND, N_RECV = 17, 9
GY, U = 1, 0
FAR = list(SLOT)[1:]
ATT = [(0, 0)] * GH
STEPS = [(b, 0) for b in range(B)] + [(0, d) for d in FAR] + ATT + [(1, d) for d in FAR] + ATT
AT0 = B + len(FAR)
AT1 = len(STEPS) - GH
NEXT1 = AT0 + GH
FETCH_HERE = (0, 2, 5, 8, NEXT1, 16, 17)
FETCH_NEXT = (0, 2, 3, 5, 6, NEXT1, 14, 17, 18)


def front_kernel(*refs):
    x_ref, gy_ref, gain_ref, lnb_ref, w_ref, wout_ref, bias_ref = refs[:7]
    all_ref, *piece_refs = refs[7:12]
    far_refs = refs[12:15]
    db_ref = refs[15]
    (wt_ref, wo_ref, qkv_ref, do_ref, pair_ref, head_ref, u_ref, dk_acc, dv_acc,
     send_sem, recv_sem, peer_sem, own_sem, pair_sem, head_sem, w_sem, osend_sem, orecv_sem) = refs[16:]
    me = lax.axis_index("sp")
    near = {bit: flip(me, bit) for bit in NEAR}
    peer = flip(me, 1)
    src = {0: me, **near}
    src[6], src[12], src[10] = flip(near[2], 4), flip(near[4], 8), flip(near[8], 2)
    src[14] = flip(src[6], 8)
    chip = me // 2
    group = chip + (chip // 4) * (7 - 2 * chip)
    mine = 4 * (me % 2) + group
    third = D // 3
    mesh_id = pl.DeviceIdType.MESH
    sends = []

    def half(b, d, h):
        return all_ref.at[b, d, pl.ds(h * TOK, TOK)]

    def descriptor(b, h, n, kind, d):
        source = target = half(b, src[d if kind else 0], h)
        if kind == 0:
            source = own_rows(b, h)
            recv, to = recv_sem.at[b, h, SLOT[d] - 1], near[d]
        elif kind == 1:
            far = [e for e in VIA if VIA[e] == d][0]
            recv, to = recv_sem.at[b, h, SLOT[far] - 1], near[far - d]
        elif kind == 2:
            j = list(LAST).index(d)
            source = target = source.at[:, pl.ds(j * third, third)]
            recv, to = recv_sem.at[b, h, 6 + j], near[LAST[d]]
        else:
            if d == 0:
                source = own_rows(b, h)
            recv, to = peer_sem.at[b, h, SLOT[d]], peer
        return pltpu.make_async_remote_copy(
            src_ref=source, dst_ref=target, send_sem=send_sem.at[b, h, n], recv_sem=recv,
            device_id=(to,), device_id_type=mesh_id)

    def send(b, h, kind, d):
        spec = (b, h, sum(1 for other in sends if other[:2] == (b, h)), kind, d)
        sends.append(spec)
        descriptor(*spec).start()

    def arrived(target, sem):
        pltpu.make_async_copy(target, target, sem).wait()

    def own_rows(b, h):
        return gy_ref.at[b] if h == GY else half(b, me, U)

    def stage0(b, h):
        for bit in NEAR:
            send(b, h, 0, bit)

    def stage0_peer(b, h):
        send(b, h, 3, 0)

    def stage1(b, h):
        for d in NEAR:
            arrived(half(b, src[d], h), recv_sem.at[b, h, SLOT[d] - 1])
            send(b, h, 1, d)
            send(b, h, 3, d)

    def stage2(b, h):
        for d in LAST:
            arrived(half(b, src[d], h), recv_sem.at[b, h, SLOT[d] - 1])
            send(b, h, 2, d)
            send(b, h, 3, d)

    def stage3(b, h):
        for j in range(3):
            arrived(half(b, src[14], h).at[:, pl.ds(j * third, third)], recv_sem.at[b, h, 6 + j])
        send(b, h, 3, 14)

    def look_up(k, values):
        return sum(jnp.where(k == i, v, 0) for i, v in enumerate(values) if v)

    def pair_of(k):
        flips = look_up(k, [d // 2 for _, d in STEPS])
        x, y, z = (chip % 2 + flips) % 2, (chip // 2 + flips // 2) % 2, (chip // 4 + flips // 4) % 2
        return look_up(k, [b for b, _ in STEPS]), x + 2 * y + 4 * z, look_up(k, [SLOT[d] for _, d in STEPS])

    def fetch(k):
        b, source, slot = pair_of(k)
        for h in range(2):
            arrived(half(b, 2 * source, h), peer_sem.at[b, h, slot])
        pair_copy(k).start()

    def pair_copy(k):
        b, source, _ = pair_of(k)
        return pltpu.make_async_copy(all_ref.at[b, pl.ds(2 * source, 2)], pair_ref.at[k % 2], pair_sem.at[k % 2])

    def among(k, steps):
        return sum(jnp.where(k == i, 1, 0) for i in steps) > 0

    def project(k):
        @pl.when(among(k, FETCH_HERE))
        def _():
            fetch(k)

        pair_copy(k).wait()

        @pl.when(among(k, FETCH_NEXT))
        def _():
            fetch(k + 1)

        b, source, _ = pair_of(k)
        pair = pair_ref.at[k % 2]
        u = jnp.concatenate([pair[0, :TOK], pair[1, :TOK]], axis=0)
        gy = jnp.concatenate([pair[0, TOK:], pair[1, TOK:]], axis=0)
        cols = aligned(source * 2 * TOK, 2 * TOK)
        qkv_ref[b, :, cols] = (dot_nt(wt_ref[...], u) + bias_ref[...]).astype(BF16)
        do_ref[b, :, cols] = dot_nt(wo_ref[...], gy).astype(BF16)

    weights = [pltpu.make_async_copy(w_ref.at[t, mine], wt_ref.at[pl.ds(t * GR, GR)], w_sem.at[t]) for t in range(3)]
    weights.append(pltpu.make_async_copy(wout_ref.at[mine], wo_ref, w_sem.at[3]))
    for c in weights:
        c.start()

    barrier = pltpu.get_barrier_semaphore()
    for d in (peer, *near.values()):
        pl.semaphore_signal(barrier, inc=1, device_id=(d,), device_id_type=mesh_id)
    pl.semaphore_wait(barrier, 4)

    stage0(0, GY)
    for b in range(B):
        load = pltpu.make_async_copy(gy_ref.at[b], pair_ref.at[b, 0, pl.ds(TOK, TOK)], own_sem.at[3 * b])
        load.start()
        x = x_ref[b].astype(F32)
        u_ref[b] = (normalize(x)[0] * gain_ref[...] + lnb_ref[...]).astype(BF16)
        store = [pltpu.make_async_copy(u_ref.at[b], half(b, me, U), own_sem.at[3 * b + 1])]
        store[0].start()
        load.wait()
        store.append(pltpu.make_async_copy(pair_ref.at[b, 0, pl.ds(TOK, TOK)], half(b, me, GY), own_sem.at[3 * b + 2]))
        store[1].start()
        for c in store:
            c.wait()
        if b == 0:
            stage0(0, U)
        stage0_peer(b, U)
        stage0_peer(b, GY)
    for c in weights:
        c.wait()

    def head_of(ref, i):
        return ref.at[aligned((i % GH) * DH, DH), aligned((i // GH) * S, S)]

    def local_copies(i):
        return [pltpu.make_async_copy(head_ref.at[i % 2, n], head_of(ref, i), head_sem.at[i % 2, n])
                for n, ref in enumerate(piece_refs)]

    def o_copies(i):
        return [pltpu.make_async_remote_copy(
            src_ref=head_of(piece_refs[0], i), dst_ref=head_of(far_refs[n], i), send_sem=osend_sem.at[i, n],
            recv_sem=orecv_sem.at[i, n], device_id=(near[bit],), device_id_type=mesh_id)
            for n, bit in enumerate(NEAR)]

    def stored(i):
        for c in local_copies(i):
            c.wait()

    def pass_on(i):
        for c in o_copies(i):
            c.start()

    def attend(i):
        b, h = i // GH, i % GH
        rows = lambda ref, t: ref.at[b, aligned(t * GR + h * DH, DH)]
        out = [head_ref.at[i % 2, n] for n in range(len(piece_refs))]
        sums = att_head(*(rows(qkv_ref, t) for t in range(3)), rows(do_ref, 0), *out, dk_acc, dv_acc)
        for t, db in enumerate(sums):
            db_ref[b, t, aligned(h * DH, DH), :] = jnp.broadcast_to(db, (DH, LANES))
        for c in local_copies(i):
            c.start()

        @pl.when(h > 0)
        def _():
            stored(i - 1)

        @pl.when(i > GH)
        def _():
            pass_on(i - 1)

    def first_o():
        stored(GH - 1)
        for i in range(GH):
            pass_on(i)

    duties = {
        2: [lambda: stage1(0, GY), lambda: stage1(0, U)],
        5: [lambda: stage2(0, GY), lambda: stage2(0, U), lambda: stage0(1, GY), lambda: stage0(1, U)],
        8: [lambda: stage3(0, GY), lambda: stage3(0, U)],
        AT0 + 1: [lambda: stage1(1, GY)],
        AT0 + 2: [lambda: stage1(1, U)],
        NEXT1: [lambda: stage2(1, GY)],
        15: [lambda: stage2(1, U)],
        17: [lambda: stage3(1, GY), lambda: stage3(1, U), first_o],
    }

    def step(k, carry):
        for at, calls in duties.items():
            @pl.when(k == at)
            def _():
                for call in calls:
                    call()

        attending = jnp.logical_or(jnp.logical_and(k >= AT0, k < NEXT1), k >= AT1)

        @pl.when(attending)
        def _():
            attend(k - jnp.where(k < NEXT1, AT0, AT1 - GH))

        @pl.when(jnp.logical_not(attending))
        def _():
            project(k)

        return carry

    lax.fori_loop(0, len(STEPS), step, 0)
    stored(B * GH - 1)
    pass_on(B * GH - 1)
    for spec in sends:
        descriptor(*spec).wait_send()
    for i in range(B * GH):
        for c in o_copies(i):
            c.wait()


def front(x_in, grad_y, gain, ln_bias, w_rows, w_out, bias):
    vmem = pl.BlockSpec(memory_space=pltpu.VMEM)
    anywhere = pl.BlockSpec(memory_space=pl.ANY)
    gathered = jax.ShapeDtypeStruct((B, NDEV, 2 * TOK, D), BF16)
    piece = jax.ShapeDtypeStruct((GR, B * S), BF16)
    return pl.pallas_call(
        front_kernel,
        in_specs=[vmem, anywhere, vmem, vmem, anywhere, anywhere, vmem],
        out_specs=[anywhere] * 8 + [vmem],
        out_shape=[gathered] + [piece] * 7 + [jax.ShapeDtypeStruct((B, 3, GR, LANES), F32)],
        scratch_shapes=[
            pltpu.VMEM((3 * GR, D), BF16),
            pltpu.VMEM((GR, D), BF16),
            pltpu.VMEM((B, 3 * GR, S), BF16),
            pltpu.VMEM((B, GR, S), BF16),
            pltpu.VMEM((2, 2, 2 * TOK, D), BF16),
            pltpu.VMEM((2, 4, DH, S), BF16),
            pltpu.VMEM((B, TOK, D), BF16),
            pltpu.VMEM((DH, S), F32),
            pltpu.VMEM((DH, S), F32),
            dma((B, 2, N_SEND)),
            dma((B, 2, N_RECV)),
            dma((B, 2, 8)),
            dma((6,)),
            dma((2,)),
            dma((2, 4)),
            dma((4,)),
            dma((B * GH, 3)),
            dma((B * GH, 3)),
        ],
        compiler_params=params(collective_id=0, has_side_effects=True),
        cost_estimate=cost(15e10, 2e8),
        name="front",
    )(x_in, grad_y, gain.reshape(1, D), ln_bias.reshape(1, D), w_rows, w_out.reshape(8, GR, D), bias)


def my_group(tbl, s):
    return aligned(tbl[3 + s] * GR, GR)


def collect_kernel(tbl, *refs):
    for s in range(4):
        for k in range(4):
            refs[-1][k * TOK:(k + 1) * TOK, my_group(tbl, s)] = refs[4 * k + s][...].T


def collect(tbl, pieces):
    spec = lambda k: pl.BlockSpec((GR, TOK), lambda i, t: (0, (k % B) * NDEV + t[1 + k // B]))
    return pl.pallas_call(
        collect_kernel,
        grid_spec=pltpu.PrefetchScalarGridSpec(
            num_scalar_prefetch=1, grid=(1,), in_specs=[spec(k) for k in range(4) for _ in pieces],
            out_specs=fixed(2 * B * TOK, CR)),
        out_shape=jax.ShapeDtypeStruct((2 * B * TOK, CR), BF16),
        compiler_params=params(),
        cost_estimate=cost(1e9, 3e6),
        name="collect",
    )(tbl, *pieces * 4)


BD = 256
SPLIT = 3


def dw_kernel(t, groups, n_in, rows_at, puts, times, tbl, x0, x1, *refs):
    pieces = refs[:4]
    outs = refs[n_in:]
    buf_ref, ex_ref = outs[:2]
    lhs_ref, own_ref, sem, own_sem, ex_sem, put_sem = outs[-6:]
    j = pl.program_id(0)
    core = tbl[0]
    extra = list(refs[4:n_in])

    @pl.when(j == 0)
    def _():
        for wait in (False, True):
            for s, piece in enumerate(pieces):
                place = tbl[3 + s] - groups[0]

                @pl.when(jnp.logical_and(place >= 0, tbl[3 + s] < groups[1]))
                def _():
                    run_all([pltpu.make_async_copy(piece, lhs_ref.at[aligned(place * GR, GR)], sem.at[s])], wait)

    def columns(step):
        return aligned(step * BD, BD)

    def own_out(step):
        src = own_ref.at[step % 2]
        start = (2 * t + core) * CR + groups[0] * GR
        rows = pl.ds(pl.multiple_of(start, GR), own_ref.shape[1])
        return (pltpu.make_async_copy(src, buf_ref.at[rows, columns(step)], own_sem.at[step % 2]),
                pltpu.make_async_copy(src, ex_ref.at[:, columns(step)], ex_sem.at[step % 2]))

    put_copies = []
    for n, (at, row_block) in enumerate(puts):
        rows = aligned((2 * row_block + 1 - core) * CR, CR)
        put_copies.append(pltpu.make_async_copy(extra.pop(0), outs[at].at[rows, columns(j)], put_sem.at[n]))
    run_all(put_copies)

    x = jnp.concatenate([ref[0, r] for ref in (x0, x1) for r in range(NDEV)], axis=0)
    res = dot_nn(lhs_ref[...], x)
    if times is not None:
        part = dot_nn(extra[0][...], extra[1][...])
        for k in range(2):
            outs[times + k][...] = part[k * B * TOK:(k + 1) * B * TOK]

    @pl.when(j >= 2)
    def _():
        run_all(own_out(j - 2), True)

    own_ref[j % 2] = res
    run_all(own_out(j))

    if rows_at is not None:
        @pl.when(j == 0)
        def _():
            for k in range(4):
                cols = aligned((k % B) * S + tbl[1 + k // B] * TOK, TOK)
                outs[rows_at][k * TOK:(k + 1) * TOK, :] = lhs_ref[:, cols].T

    run_all(put_copies, True)

    @pl.when(j == pl.num_programs(0) - 1)
    def _():
        run_all(own_out(j - 1) + own_out(j), True)


def weight_grad(tbl, gathered, pieces, t, which, out_rows, prev=None, rows=True, puts=(), times=None, groups=(0, 4)):
    n_rows = (groups[1] - groups[0]) * GR
    anywhere = pl.BlockSpec(memory_space=pl.ANY)
    x_spec = lambda b: pl.BlockSpec((1, NDEV, TOK, BD), lambda j, t: (b, 0, which, j))
    ins = [(x_spec(b), gathered) for b in range(B)] + [(anywhere, p) for p in pieces]
    outs = [(anywhere, (out_rows, D), F32), (anywhere, (n_rows, D), F32)]
    rows_at = times_at = None
    put_at = []
    whole = fixed(2 * B * TOK, CR)
    if rows:
        rows_at = len(outs)
        outs.append((whole, (2 * B * TOK, CR), BF16))
    if times is not None:
        times_at = len(outs)
        outs += [(by_column(B * TOK, BD), (B * TOK, D), F32)] * 2
    ins += [(by_column(CR, BD), block) for block, *_ in puts]
    if times is not None:
        ins.append((whole, times[0]))
        ins.append((pl.BlockSpec((CR, BD), lambda j, t: (2 * times[2] + t[0], j)), times[1]))
    alias = {}
    if prev is not None:
        alias[1 + len(ins)] = 0
        ins.append((anywhere, prev))
    for _, row_block, buffer in puts:
        put_at.append((0 if buffer is None else len(outs), row_block))
        if buffer is not None:
            alias[1 + len(ins)] = len(outs)
            ins.append((anywhere, buffer))
            outs.append((anywhere, buffer.shape, F32))
    return pl.pallas_call(
        functools.partial(dw_kernel, t, groups, len(ins) - B, rows_at, put_at, times_at),
        grid_spec=pltpu.PrefetchScalarGridSpec(
            num_scalar_prefetch=1,
            grid=(D // BD,),
            in_specs=[spec for spec, _ in ins],
            out_specs=[spec for spec, *_ in outs],
            scratch_shapes=[
                pltpu.VMEM((n_rows, B * S), BF16),
                pltpu.VMEM((2, n_rows, BD), F32),
                dma((4,)), dma((2,)), dma((2,)), dma((2,)),
            ]),
        out_shape=[jax.ShapeDtypeStruct(*shape) for _, *shape in outs],
        input_output_aliases=alias,
        compiler_params=params(),
        cost_estimate=cost(2 * n_rows * D * B * S, 75e6),
        name="weight_grad",
    )(tbl, *(arg for _, arg in ins))


CB = 512


def contract_kernel(n, *refs):
    rows = jnp.concatenate([r[...] for r in refs[1:1 + n]], axis=1)
    weight = jnp.concatenate([r[...] for r in refs[1 + n:1 + 2 * n]], axis=0)
    acc = dot_nn(rows, weight)
    for k, prev in enumerate(refs[1 + 2 * n:-2]):
        refs[k - 2][...] = acc[k * B * TOK:(k + 1) * B * TOK] + prev[...]


def contract(tbl, rows, weight, blocks, prev):
    out = by_column(B * TOK, CB)
    w_spec = lambda block: pl.BlockSpec((CR, CB), lambda i, t: (2 * block + t[0], i))
    n = len(blocks)
    return pl.pallas_call(
        functools.partial(contract_kernel, n),
        grid_spec=pltpu.PrefetchScalarGridSpec(
            num_scalar_prefetch=1,
            grid=(D // CB,),
            in_specs=[fixed(2 * B * TOK, CR)] * n
            + [w_spec(block) for block in blocks] + [out] * 2,
            out_specs=[out] * 2),
        out_shape=[jax.ShapeDtypeStruct((B * TOK, D), F32)] * 2,
        compiler_params=params(),
        cost_estimate=cost(2 * B * TOK * D * D * n, 22e6),
        name="contract",
    )(tbl, *rows, *[weight] * n, *prev)


def finish_kernel(du_own, du_peer, x_ref, gy_ref, db_ref, gain_ref, gx_ref, sums_ref):
    x_hat, inv_std = normalize(x_ref[0].astype(F32))
    du = (du_own[...] + du_peer[...]).astype(BF16).astype(F32)
    gy = gy_ref[0].astype(F32)
    grad_hat = du * gain_ref[...]
    centered = grad_hat - jnp.mean(grad_hat, **LAST_DIM)
    gx_ref[0] = (gy + inv_std * (centered - x_hat * jnp.mean(grad_hat * x_hat, **LAST_DIM))).astype(BF16)

    @pl.when(pl.program_id(0) == 0)
    def _():
        sums_ref[...] = db_ref[...]

    for k, val in enumerate((du * x_hat, du, gy)):
        sums_ref[k:k + 1, :] += jnp.sum(val, **ROWS)


def finish_y_kernel(y_own, y_peer, x_ref, b_ref, y_ref):
    y_ref[0] = (x_ref[0].astype(F32) + (y_own[...] + y_peer[...] + b_ref[...])).astype(BF16)


def finish(kernel, partials, acts, vector, sums=None):
    more = [] if sums is None else [sums]
    act = pl.BlockSpec((1, TOK, D), lambda b: (b, 0, 0))
    grad = jax.ShapeDtypeStruct((B, TOK, D), BF16)
    return pl.pallas_call(
        kernel,
        grid=(B,),
        in_specs=[pl.BlockSpec((TOK, D), lambda b: (b, 0))] * len(partials) + [act] * len(acts)
        + [fixed(8, D) for _ in more] + [fixed(1, D)],
        out_specs=[act] + [fixed(8, D) for _ in more],
        out_shape=[grad] + [jax.ShapeDtypeStruct((8, D), F32) for _ in more],
        compiler_params=params(),
        cost_estimate=cost(1e8, 1e7),
        name="finish",
    )(*partials, *acts, *more, vector.reshape(1, D))


def solution(mesh):
    def permute(a, bit):
        return lax.ppermute(a, "sp", [(i, i ^ bit) for i in range(NDEV)])

    def block(x_in, grad_y, ln_gain, ln_bias, w_qkv, b_qkv, w_out, b_out):
        me = lax.axis_index("sp")
        core, chip = me % 2, me // 2
        group = lambda c: jnp.where(c < 4, c, 7 - c)
        groups = [group(chip ^ d) for d in (0, 1, 2, 4)]
        tbl = jnp.stack([core, me, me ^ 1] + groups).astype(jnp.int32)
        mine = 4 * core + groups[0]

        flat_w = jnp.transpose(w_qkv, (1, 2, 3, 0)).reshape(3 * D, D)
        bias = lax.dynamic_slice_in_dim(b_qkv.reshape(3, 8, GR), mine, 1, axis=1).reshape(3 * GR, 1)
        gathered, o, dq, dk, dv, *far_o, db = front(
            x_in, grad_y, ln_gain, ln_bias, flat_w.reshape(3, 8, GR, D), w_out, bias)

        pieces = {"o": [o] + far_o}
        for name, piece in (("v", dv), ("k", dk), ("q", dq)):
            pieces[name] = [piece] + [permute(piece, bit) for bit in NEAR]

        def swap(a):
            return permute(a, 1)

        def grad(name, *args, **kw):
            return weight_grad(tbl, gathered, pieces[name[0]], *args, **kw)

        gwo, ex_o, rows_o = grad("o", 0, GY, D)
        ex_o = swap(ex_o)
        gwq, ex_v, rows_v, y_own, y_peer = grad("v", 2, U, 3 * D, times=(rows_o, w_out.reshape(D, D), 0))
        y_peer = swap(y_peer)
        ex_v = swap(ex_v)
        gwq, ex_k, rows_k, *du, gwo = grad("k", 1, U, 3 * D, gwq, puts=[(ex_o, 0, gwo)], times=(rows_v, flat_w, 2))
        rows_q = collect(tbl, pieces["q"])
        ex_k = swap(ex_k)
        du_own, du_peer = contract(tbl, [rows_k, rows_q], flat_w, [1, 0], du)
        du_peer = swap(du_peer)
        y_out, = finish(finish_y_kernel, [y_own, y_peer], [x_in], b_out)
        db = jnp.where(chip < 4, db[0, :, :, 0] + db[1, :, :, 0], 0.0).reshape(3, 1, GR)
        sums = lax.dynamic_update_slice(jnp.zeros((8, 8, GR), F32), db, (3, mine, 0)).reshape(8, D)
        grad_x, sums = finish(finish_kernel, [du_own, du_peer], [x_in, grad_y], ln_gain, sums)
        parts = [(0, SPLIT), (SPLIT, 4)]
        gwq, ex_q0 = grad("q0", 0, U, 3 * D, gwq, rows=False, puts=[(ex_v, 2, None), (ex_k, 1, None)], groups=parts[0])
        ex_q0 = swap(ex_q0)
        gwq, ex_q1 = grad("q1", 0, U, 3 * D, gwq, rows=False, groups=parts[1])
        ex_q1 = swap(ex_q1)
        for bit in (1, *NEAR):
            sums = sums + permute(sums, bit)
        for ex, part in ((ex_q0, parts[0]), (ex_q1, parts[1])):
            gwq = lax.dynamic_update_slice(gwq, ex, ((1 - core) * CR + part[0] * GR, 0))

        grad_w_qkv = jnp.transpose(gwq.reshape(3, NH, DH, D), (3, 0, 1, 2))
        grad_b_qkv = sums[3:6].reshape(3, NH, DH)
        return y_out, grad_x, sums[0], sums[1], grad_w_qkv, grad_b_qkv, gwo.reshape(NH, DH, D), sums[2]

    seq, rep = P(None, "sp", None), P()
    specs = (seq, seq) + (rep,) * 6
    return jax.shard_map(block, mesh=mesh, in_specs=specs, out_specs=specs, check_vma=False)
```

```python
import functools
import math

import jax
import jax.numpy as jnp
from jax import lax
from jax.experimental import pallas as pl
from jax.experimental.pallas import tpu as pltpu
from jax.sharding import PartitionSpec as P


LN_EPS = 1e-5
F32 = jnp.float32
BF16 = jnp.bfloat16
VMEM_LIMIT = 64 * 1024 * 1024 - 65536

B, S, D, NH, DH = 2, 2048, 3072, 32, 96
NDEV = 16
TOK = S // NDEV
GH = 4
GR = GH * DH
CR = 4 * GR
SCALE = DH ** -0.5
BQ = 512
LANES = 128


def dot_nt(a, b):
    return lax.dot_general(a, b, (((1,), (1,)), ((), ())), preferred_element_type=F32)


def dot_nn(a, b):
    return jnp.dot(a, b, preferred_element_type=F32)


def params(**kw):
    return pltpu.CompilerParams(vmem_limit_bytes=VMEM_LIMIT, **kw)


def cost(flops, moved):
    return pl.CostEstimate(flops=int(flops), bytes_accessed=int(moved), transcendentals=0)


ROWS = dict(axis=0, keepdims=True)
LAST_DIM = dict(axis=-1, keepdims=True)


def normalize(x):
    centered = x - jnp.mean(x, **LAST_DIM)
    inv_std = lax.rsqrt(jnp.mean(centered * centered, **LAST_DIM) + LN_EPS)
    return centered * inv_std, inv_std


def fixed(*shape):
    return pl.BlockSpec(shape, lambda *_: (0,) * len(shape))


def by_column(*shape):
    return pl.BlockSpec(shape, lambda j, *_: (0, j))


def aligned(start, size):
    return pl.ds(pl.multiple_of(start, size), size)


def run_all(copies, wait=False):
    for c in copies:
        c.wait() if wait else c.start()


dma = pltpu.SemaphoreType.DMA


def flip(index, bit):
    return index + bit * (1 - 2 * ((index // bit) % 2))


def att_head(q_ref, k_ref, v_ref, do_ref, o_ref, dq_ref, dk_ref, dv_ref, dk_acc, dv_acc):
    to_exp2 = SCALE * math.log2(math.e)
    k_t = k_ref[...]
    v_t = v_ref[...]
    k_n = k_t.T
    v_n = v_t.T
    db_q = jnp.zeros((DH, 1), F32)
    for i in reversed(range(S // BQ)):
        keys = (i + 1) * BQ
        cols = slice(i * BQ, keys)
        q = q_ref[:, cols]
        do = do_ref[:, cols]
        s = dot_nn(k_n[:keys], q)
        row = lax.broadcasted_iota(jnp.int32, (BQ, BQ), 0)
        col = lax.broadcasted_iota(jnp.int32, (BQ, BQ), 1)
        s_diag = jnp.where(row <= col, s[keys - BQ:], -1e30)
        s = jnp.concatenate([s[:keys - BQ], s_diag], axis=0) if i else s_diag
        m = jnp.max(s, **ROWS)
        p = jnp.exp2((s - m) * to_exp2)
        p = p * (1.0 / jnp.sum(p, **ROWS))
        p_low = p.astype(BF16)
        o = dot_nn(v_t[:, :keys], p_low)
        o_ref[:, cols] = o.astype(BF16)
        dp = dot_nn(v_n[:keys], do).astype(BF16).astype(F32)
        row_dot = jnp.sum(o * do.astype(F32), **ROWS)
        ds = (p * (dp - row_dot)).astype(BF16)
        dq = (dot_nn(k_t[:, :keys], ds) * SCALE).astype(BF16)
        dq_ref[:, cols] = dq
        db_q += jnp.sum(dq.astype(F32), **LAST_DIM)
        dk = dot_nt(q, ds)
        dv = dot_nt(do, p_low)
        if keys == S:
            dk_acc[...] = dk
            dv_acc[...] = dv
        else:
            dk_acc[:, :keys] += dk
            dv_acc[:, :keys] += dv
    dk = (dk_acc[...] * SCALE).astype(BF16)
    dv = dv_acc[...].astype(BF16)
    dk_ref[...] = dk
    dv_ref[...] = dv
    return db_q, jnp.sum(dk.astype(F32), **LAST_DIM), jnp.sum(dv.astype(F32), **LAST_DIM)


NEAR = (2, 4, 8)
VIA = {6: 4, 12: 8, 10: 2}
LAST = {12: 2, 10: 4, 6: 8}
SLOT = {d: i for i, d in enumerate((0, 2, 4, 8, 6, 12, 10, 14))}
N_SEND, N_RECV = 17, 9
GY, U = 1, 0
FAR = list(SLOT)[1:]
ATT = [(0, 0)] * GH
STEPS = [(b, 0) for b in range(B)] + [(0, d) for d in FAR] + ATT + [(1, d) for d in FAR] + ATT
AT0 = B + len(FAR)
AT1 = len(STEPS) - GH
NEXT1 = AT0 + GH
FETCH_HERE = (0, 2, 5, 8, NEXT1, 16, 17)
FETCH_NEXT = (0, 2, 3, 5, 6, NEXT1, 14, 17, 18)


def front_kernel(*refs):
    x_ref, gy_ref, gain_ref, lnb_ref, w_ref, wout_ref, bias_ref = refs[:7]
    all_ref, *piece_refs = refs[7:12]
    far_refs = refs[12:15]
    db_ref = refs[15]
    (wt_ref, wo_ref, qkv_ref, do_ref, pair_ref, head_ref, u_ref, dk_acc, dv_acc,
     send_sem, recv_sem, peer_sem, own_sem, pair_sem, head_sem, w_sem, osend_sem, orecv_sem) = refs[16:]
    me = lax.axis_index("sp")
    near = {bit: flip(me, bit) for bit in NEAR}
    peer = flip(me, 1)
    src = {0: me, **near}
    src[6], src[12], src[10] = flip(near[2], 4), flip(near[4], 8), flip(near[8], 2)
    src[14] = flip(src[6], 8)
    chip = me // 2
    group = chip + (chip // 4) * (7 - 2 * chip)
    mine = 4 * (me % 2) + group
    third = D // 3
    mesh_id = pl.DeviceIdType.MESH
    sends = []

    def half(b, d, h):
        return all_ref.at[b, d, pl.ds(h * TOK, TOK)]

    def descriptor(b, h, n, kind, d):
        source = target = half(b, src[d if kind else 0], h)
        if kind == 0:
            source = own_rows(b, h)
            recv, to = recv_sem.at[b, h, SLOT[d] - 1], near[d]
        elif kind == 1:
            far = [e for e in VIA if VIA[e] == d][0]
            recv, to = recv_sem.at[b, h, SLOT[far] - 1], near[far - d]
        elif kind == 2:
            j = list(LAST).index(d)
            source = target = source.at[:, pl.ds(j * third, third)]
            recv, to = recv_sem.at[b, h, 6 + j], near[LAST[d]]
        else:
            if d == 0:
                source = own_rows(b, h)
            recv, to = peer_sem.at[b, h, SLOT[d]], peer
        return pltpu.make_async_remote_copy(
            src_ref=source, dst_ref=target, send_sem=send_sem.at[b, h, n], recv_sem=recv,
            device_id=(to,), device_id_type=mesh_id)

    def send(b, h, kind, d):
        spec = (b, h, sum(1 for other in sends if other[:2] == (b, h)), kind, d)
        sends.append(spec)
        descriptor(*spec).start()

    def arrived(target, sem):
        pltpu.make_async_copy(target, target, sem).wait()

    def own_rows(b, h):
        return gy_ref.at[b] if h == GY else half(b, me, U)

    def stage0(b, h):
        for bit in NEAR:
            send(b, h, 0, bit)

    def stage0_peer(b, h):
        send(b, h, 3, 0)

    def stage1(b, h):
        for d in NEAR:
            arrived(half(b, src[d], h), recv_sem.at[b, h, SLOT[d] - 1])
            send(b, h, 1, d)
            send(b, h, 3, d)

    def stage2(b, h):
        for d in LAST:
            arrived(half(b, src[d], h), recv_sem.at[b, h, SLOT[d] - 1])
            send(b, h, 2, d)
            send(b, h, 3, d)

    def stage3(b, h):
        for j in range(3):
            arrived(half(b, src[14], h).at[:, pl.ds(j * third, third)], recv_sem.at[b, h, 6 + j])
        send(b, h, 3, 14)

    def look_up(k, values):
        return sum(jnp.where(k == i, v, 0) for i, v in enumerate(values) if v)

    def pair_of(k):
        flips = look_up(k, [d // 2 for _, d in STEPS])
        x, y, z = (chip % 2 + flips) % 2, (chip // 2 + flips // 2) % 2, (chip // 4 + flips // 4) % 2
        return look_up(k, [b for b, _ in STEPS]), x + 2 * y + 4 * z, look_up(k, [SLOT[d] for _, d in STEPS])

    def fetch(k):
        b, source, slot = pair_of(k)
        for h in range(2):
            arrived(half(b, 2 * source, h), peer_sem.at[b, h, slot])
        pair_copy(k).start()

    def pair_copy(k):
        b, source, _ = pair_of(k)
        return pltpu.make_async_copy(all_ref.at[b, pl.ds(2 * source, 2)], pair_ref.at[k % 2], pair_sem.at[k % 2])

    def among(k, steps):
        return sum(jnp.where(k == i, 1, 0) for i in steps) > 0

    def project(k):
        @pl.when(among(k, FETCH_HERE))
        def _():
            fetch(k)

        pair_copy(k).wait()

        @pl.when(among(k, FETCH_NEXT))
        def _():
            fetch(k + 1)

        b, source, _ = pair_of(k)
        pair = pair_ref.at[k % 2]
        u = jnp.concatenate([pair[0, :TOK], pair[1, :TOK]], axis=0)
        gy = jnp.concatenate([pair[0, TOK:], pair[1, TOK:]], axis=0)
        cols = aligned(source * 2 * TOK, 2 * TOK)
        qkv_ref[b, :, cols] = (dot_nt(wt_ref[...], u) + bias_ref[...]).astype(BF16)
        do_ref[b, :, cols] = dot_nt(wo_ref[...], gy).astype(BF16)

    weights = [pltpu.make_async_copy(w_ref.at[t, mine], wt_ref.at[pl.ds(t * GR, GR)], w_sem.at[t]) for t in range(3)]
    weights.append(pltpu.make_async_copy(wout_ref.at[mine], wo_ref, w_sem.at[3]))
    for c in weights:
        c.start()

    barrier = pltpu.get_barrier_semaphore()
    for d in (peer, *near.values()):
        pl.semaphore_signal(barrier, inc=1, device_id=(d,), device_id_type=mesh_id)
    pl.semaphore_wait(barrier, 4)

    stage0(0, GY)
    for b in range(B):
        load = pltpu.make_async_copy(gy_ref.at[b], pair_ref.at[b, 0, pl.ds(TOK, TOK)], own_sem.at[3 * b])
        load.start()
        x = x_ref[b].astype(F32)
        u_ref[b] = (normalize(x)[0] * gain_ref[...] + lnb_ref[...]).astype(BF16)
        store = [pltpu.make_async_copy(u_ref.at[b], half(b, me, U), own_sem.at[3 * b + 1])]
        store[0].start()
        load.wait()
        store.append(pltpu.make_async_copy(pair_ref.at[b, 0, pl.ds(TOK, TOK)], half(b, me, GY), own_sem.at[3 * b + 2]))
        store[1].start()
        for c in store:
            c.wait()
        if b == 0:
            stage0(0, U)
        stage0_peer(b, U)
        stage0_peer(b, GY)
    for c in weights:
        c.wait()

    def head_of(ref, i):
        return ref.at[aligned((i % GH) * DH, DH), aligned((i // GH) * S, S)]

    def local_copies(i):
        return [pltpu.make_async_copy(head_ref.at[i % 2, n], head_of(ref, i), head_sem.at[i % 2, n])
                for n, ref in enumerate(piece_refs)]

    def o_copies(i):
        return [pltpu.make_async_remote_copy(
            src_ref=head_of(piece_refs[0], i), dst_ref=head_of(far_refs[n], i), send_sem=osend_sem.at[i, n],
            recv_sem=orecv_sem.at[i, n], device_id=(near[bit],), device_id_type=mesh_id)
            for n, bit in enumerate(NEAR)]

    def stored(i):
        for c in local_copies(i):
            c.wait()

    def pass_on(i):
        for c in o_copies(i):
            c.start()

    def attend(i):
        b, h = i // GH, i % GH
        rows = lambda ref, t: ref.at[b, aligned(t * GR + h * DH, DH)]
        out = [head_ref.at[i % 2, n] for n in range(len(piece_refs))]
        sums = att_head(*(rows(qkv_ref, t) for t in range(3)), rows(do_ref, 0), *out, dk_acc, dv_acc)
        for t, db in enumerate(sums):
            db_ref[b, t, aligned(h * DH, DH), :] = jnp.broadcast_to(db, (DH, LANES))
        for c in local_copies(i):
            c.start()

        @pl.when(h > 0)
        def _():
            stored(i - 1)

        @pl.when(i > GH)
        def _():
            pass_on(i - 1)

    def first_o():
        stored(GH - 1)
        for i in range(GH):
            pass_on(i)

    duties = {
        2: [lambda: stage1(0, GY), lambda: stage1(0, U)],
        5: [lambda: stage2(0, GY), lambda: stage2(0, U), lambda: stage0(1, GY), lambda: stage0(1, U)],
        8: [lambda: stage3(0, GY), lambda: stage3(0, U)],
        AT0 + 1: [lambda: stage1(1, GY)],
        AT0 + 2: [lambda: stage1(1, U)],
        NEXT1: [lambda: stage2(1, GY)],
        15: [lambda: stage2(1, U)],
        17: [lambda: stage3(1, GY), lambda: stage3(1, U), first_o],
    }

    def step(k, carry):
        for at, calls in duties.items():
            @pl.when(k == at)
            def _():
                for call in calls:
                    call()

        attending = jnp.logical_or(jnp.logical_and(k >= AT0, k < NEXT1), k >= AT1)

        @pl.when(attending)
        def _():
            attend(k - jnp.where(k < NEXT1, AT0, AT1 - GH))

        @pl.when(jnp.logical_not(attending))
        def _():
            project(k)

        return carry

    lax.fori_loop(0, len(STEPS), step, 0)
    stored(B * GH - 1)
    pass_on(B * GH - 1)
    for spec in sends:
        descriptor(*spec).wait_send()
    for i in range(B * GH):
        for c in o_copies(i):
            c.wait()


def front(x_in, grad_y, gain, ln_bias, w_rows, w_out, bias):
    vmem = pl.BlockSpec(memory_space=pltpu.VMEM)
    anywhere = pl.BlockSpec(memory_space=pl.ANY)
    gathered = jax.ShapeDtypeStruct((B, NDEV, 2 * TOK, D), BF16)
    piece = jax.ShapeDtypeStruct((GR, B * S), BF16)
    return pl.pallas_call(
        front_kernel,
        in_specs=[vmem, anywhere, vmem, vmem, anywhere, anywhere, vmem],
        out_specs=[anywhere] * 8 + [vmem],
        out_shape=[gathered] + [piece] * 7 + [jax.ShapeDtypeStruct((B, 3, GR, LANES), F32)],
        scratch_shapes=[
            pltpu.VMEM((3 * GR, D), BF16),
            pltpu.VMEM((GR, D), BF16),
            pltpu.VMEM((B, 3 * GR, S), BF16),
            pltpu.VMEM((B, GR, S), BF16),
            pltpu.VMEM((2, 2, 2 * TOK, D), BF16),
            pltpu.VMEM((2, 4, DH, S), BF16),
            pltpu.VMEM((B, TOK, D), BF16),
            pltpu.VMEM((DH, S), F32),
            pltpu.VMEM((DH, S), F32),
            dma((B, 2, N_SEND)),
            dma((B, 2, N_RECV)),
            dma((B, 2, 8)),
            dma((6,)),
            dma((2,)),
            dma((2, 4)),
            dma((4,)),
            dma((B * GH, 3)),
            dma((B * GH, 3)),
        ],
        compiler_params=params(collective_id=0, has_side_effects=True),
        cost_estimate=cost(15e10, 2e8),
        name="front",
    )(x_in, grad_y, gain.reshape(1, D), ln_bias.reshape(1, D), w_rows, w_out.reshape(8, GR, D), bias)


def my_group(tbl, s):
    return aligned(tbl[3 + s] * GR, GR)


def collect_kernel(tbl, *refs):
    for s in range(4):
        for k in range(4):
            refs[-1][k * TOK:(k + 1) * TOK, my_group(tbl, s)] = refs[4 * k + s][...].T


def collect(tbl, pieces):
    spec = lambda k: pl.BlockSpec((GR, TOK), lambda i, t: (0, (k % B) * NDEV + t[1 + k // B]))
    return pl.pallas_call(
        collect_kernel,
        grid_spec=pltpu.PrefetchScalarGridSpec(
            num_scalar_prefetch=1, grid=(1,), in_specs=[spec(k) for k in range(4) for _ in pieces],
            out_specs=fixed(2 * B * TOK, CR)),
        out_shape=jax.ShapeDtypeStruct((2 * B * TOK, CR), BF16),
        compiler_params=params(),
        cost_estimate=cost(1e9, 3e6),
        name="collect",
    )(tbl, *pieces * 4)


BD = 256


def dw_kernel(t, n_in, parts, rows_at, puts, tbl, x0, x1, *refs):
    pieces = refs[:4]
    outs = refs[n_in:]
    buf_ref, *ex_refs = outs[:1 + len(parts)]
    lhs_ref, own_ref, sem, own_sem, ex_sem, put_sem = outs[-6:]
    j = pl.program_id(0)
    core = tbl[0]
    extra = list(refs[4:n_in])

    @pl.when(j == 0)
    def _():
        copies = [pltpu.make_async_copy(p, lhs_ref.at[my_group(tbl, s)], sem.at[s]) for s, p in enumerate(pieces)]
        run_all(copies)
        run_all(copies, True)

    def columns(step):
        return aligned(step * BD, BD)

    def own_out(step, wait=False):
        src = own_ref.at[step % 2]
        run_all([pltpu.make_async_copy(
            src, buf_ref.at[aligned((2 * t + core) * CR, CR), columns(step)], own_sem.at[step % 2])], wait)
        for (start, stop), ex_ref in zip(parts, ex_refs):
            @pl.when(jnp.logical_and(step * BD >= start, step * BD < stop))
            def _():
                cols = columns(step - start // BD)
                run_all([pltpu.make_async_copy(src, ex_ref.at[:, cols], ex_sem.at[step % 2])], wait)

    put_copies = []
    for n, (at, row_block) in enumerate(puts):
        rows = aligned((2 * row_block + 1 - core) * CR, CR)
        put_copies.append(pltpu.make_async_copy(extra.pop(0), outs[at].at[rows, columns(j)], put_sem.at[n]))
    run_all(put_copies)

    x = jnp.concatenate([ref[0, r] for ref in (x0, x1) for r in range(NDEV)], axis=0)
    res = dot_nn(lhs_ref[...], x)

    @pl.when(j >= 2)
    def _():
        own_out(j - 2, True)

    own_ref[j % 2] = res
    own_out(j)

    if rows_at is not None:
        @pl.when(j == 0)
        def _():
            for k in range(4):
                cols = aligned((k % B) * S + tbl[1 + k // B] * TOK, TOK)
                outs[rows_at][k * TOK:(k + 1) * TOK, :] = lhs_ref[:, cols].T

    run_all(put_copies, True)

    @pl.when(j == pl.num_programs(0) - 1)
    def _():
        own_out(j - 1, True)
        own_out(j, True)


def weight_grad(tbl, gathered, pieces, t, which, out_rows, prev=None, rows=True, puts=(), parts=((0, D),)):
    anywhere = pl.BlockSpec(memory_space=pl.ANY)
    x_spec = lambda b: pl.BlockSpec((1, NDEV, TOK, BD), lambda j, t: (b, 0, which, j))
    ins = [(x_spec(b), gathered) for b in range(B)] + [(anywhere, p) for p in pieces]
    outs = [(anywhere, (out_rows, D), F32)] + [(anywhere, (CR, stop - start), F32) for start, stop in parts]
    rows_at = None
    put_at = []
    if rows:
        rows_at = len(outs)
        outs.append((fixed(2 * B * TOK, CR), (2 * B * TOK, CR), BF16))
    ins += [(by_column(CR, BD), block) for block, *_ in puts]
    alias = {}
    if prev is not None:
        alias[1 + len(ins)] = 0
        ins.append((anywhere, prev))
    for _, row_block, buffer in puts:
        put_at.append((0 if buffer is None else len(outs), row_block))
        if buffer is not None:
            alias[1 + len(ins)] = len(outs)
            ins.append((anywhere, buffer))
            outs.append((anywhere, buffer.shape, F32))
    return pl.pallas_call(
        functools.partial(dw_kernel, t, len(ins) - B, parts, rows_at, put_at),
        grid_spec=pltpu.PrefetchScalarGridSpec(
            num_scalar_prefetch=1,
            grid=(D // BD,),
            in_specs=[spec for spec, _ in ins],
            out_specs=[spec for spec, *_ in outs],
            scratch_shapes=[
                pltpu.VMEM((CR, B * S), BF16),
                pltpu.VMEM((2, CR, BD), F32),
                dma((4,)), dma((2,)), dma((2,)), dma((2,)),
            ]),
        out_shape=[jax.ShapeDtypeStruct(*shape) for _, *shape in outs],
        input_output_aliases=alias,
        compiler_params=params(),
        cost_estimate=cost(2 * CR * D * B * S, 75e6),
        name="weight_grad",
    )(tbl, *(arg for _, arg in ins))


CB = 512


def contract_kernel(n, *refs):
    rows = jnp.concatenate([r[...] for r in refs[1:1 + n]], axis=1)
    weight = jnp.concatenate([r[...] for r in refs[1 + n:1 + 2 * n]], axis=0)
    acc = dot_nn(rows, weight)
    prev = refs[1 + 2 * n:-2]
    for k in range(2):
        part = acc[k * B * TOK:(k + 1) * B * TOK]
        refs[k - 2][...] = part + prev[k][...] if prev else part


def contract(tbl, rows, weight, blocks, prev=()):
    out = by_column(B * TOK, CB)
    w_spec = lambda block: pl.BlockSpec((CR, CB), lambda i, t: (2 * block + t[0], i))
    n = len(blocks)
    return pl.pallas_call(
        functools.partial(contract_kernel, n),
        grid_spec=pltpu.PrefetchScalarGridSpec(
            num_scalar_prefetch=1,
            grid=(D // CB,),
            in_specs=[fixed(2 * B * TOK, CR)] * n
            + [w_spec(block) for block in blocks] + [out] * len(prev),
            out_specs=[out] * 2),
        out_shape=[jax.ShapeDtypeStruct((B * TOK, D), F32)] * 2,
        compiler_params=params(),
        cost_estimate=cost(2 * B * TOK * D * D * n, 22e6),
        name="contract",
    )(tbl, *rows, *[weight] * n, *prev)


def finish_kernel(du_own, du_peer, x_ref, gy_ref, db_ref, gain_ref, gx_ref, sums_ref):
    x_hat, inv_std = normalize(x_ref[0].astype(F32))
    du = (du_own[...] + du_peer[...]).astype(BF16).astype(F32)
    gy = gy_ref[0].astype(F32)
    grad_hat = du * gain_ref[...]
    centered = grad_hat - jnp.mean(grad_hat, **LAST_DIM)
    gx_ref[0] = (gy + inv_std * (centered - x_hat * jnp.mean(grad_hat * x_hat, **LAST_DIM))).astype(BF16)

    @pl.when(pl.program_id(0) == 0)
    def _():
        sums_ref[...] = db_ref[...]

    for k, val in enumerate((du * x_hat, du, gy)):
        sums_ref[k:k + 1, :] += jnp.sum(val, **ROWS)


def finish_y_kernel(y_own, y_peer, x_ref, b_ref, y_ref):
    y_ref[0] = (x_ref[0].astype(F32) + (y_own[...] + y_peer[...] + b_ref[...])).astype(BF16)


def finish(kernel, partials, acts, vector, sums=None):
    more = [] if sums is None else [sums]
    act = pl.BlockSpec((1, TOK, D), lambda b: (b, 0, 0))
    grad = jax.ShapeDtypeStruct((B, TOK, D), BF16)
    return pl.pallas_call(
        kernel,
        grid=(B,),
        in_specs=[pl.BlockSpec((TOK, D), lambda b: (b, 0))] * len(partials) + [act] * len(acts)
        + [fixed(8, D) for _ in more] + [fixed(1, D)],
        out_specs=[act] + [fixed(8, D) for _ in more],
        out_shape=[grad] + [jax.ShapeDtypeStruct((8, D), F32) for _ in more],
        compiler_params=params(),
        cost_estimate=cost(1e8, 1e7),
        name="finish",
    )(*partials, *acts, *more, vector.reshape(1, D))


def solution(mesh):
    def permute(a, bit):
        return lax.ppermute(a, "sp", [(i, i ^ bit) for i in range(NDEV)])

    def block(x_in, grad_y, ln_gain, ln_bias, w_qkv, b_qkv, w_out, b_out):
        me = lax.axis_index("sp")
        core, chip = me % 2, me // 2
        group = lambda c: jnp.where(c < 4, c, 7 - c)
        groups = [group(chip ^ d) for d in (0, 1, 2, 4)]
        tbl = jnp.stack([core, me, me ^ 1] + groups).astype(jnp.int32)
        mine = 4 * core + groups[0]

        flat_w = jnp.transpose(w_qkv, (1, 2, 3, 0)).reshape(3 * D, D)
        bias = lax.dynamic_slice_in_dim(b_qkv.reshape(3, 8, GR), mine, 1, axis=1).reshape(3 * GR, 1)
        gathered, o, dq, dk, dv, *far_o, db = front(
            x_in, grad_y, ln_gain, ln_bias, flat_w.reshape(3, 8, GR, D), w_out, bias)

        pieces = {"o": [o] + far_o}
        for name, piece in (("v", dv), ("k", dk), ("q", dq)):
            pieces[name] = [piece] + [permute(piece, bit) for bit in NEAR]

        def swap(a):
            return permute(a, 1)

        def grad(name, *args, **kw):
            return weight_grad(tbl, gathered, pieces[name[0]], *args, **kw)

        def rows_times(*args):
            return contract(tbl, *args)

        gwo, ex_o, rows_o = grad("o", 0, GY, D)
        y_own, y_peer = rows_times([rows_o], w_out.reshape(D, D), [0])
        y_peer = swap(y_peer)
        ex_o = swap(ex_o)
        gwq, ex_v, rows_v = grad("v", 2, U, 3 * D)
        ex_v = swap(ex_v)
        du = rows_times([rows_v], flat_w, [2])
        gwq, ex_k, rows_k, gwo = grad("k", 1, U, 3 * D, gwq, puts=[(ex_o, 0, gwo)])
        ex_k = swap(ex_k)
        rows_q = collect(tbl, pieces["q"])
        du_own, du_peer = rows_times([rows_k, rows_q], flat_w, [1, 0], du)
        du_peer = swap(du_peer)
        parts = ((0, 2 * D // 3), (2 * D // 3, D))
        gwq, *ex_q = grad("q", 0, U, 3 * D, gwq, rows=False, puts=[(ex_v, 2, None), (ex_k, 1, None)], parts=parts)
        ex_q = [swap(ex) for ex in ex_q]
        y_out, = finish(finish_y_kernel, [y_own, y_peer], [x_in], b_out)
        db = jnp.where(chip < 4, db[0, :, :, 0] + db[1, :, :, 0], 0.0).reshape(3, 1, GR)
        sums = lax.dynamic_update_slice(jnp.zeros((8, 8, GR), F32), db, (3, mine, 0)).reshape(8, D)
        grad_x, sums = finish(finish_kernel, [du_own, du_peer], [x_in, grad_y], ln_gain, sums)
        for bit in (*NEAR, 1):
            sums = sums + permute(sums, bit)
        for n, ex in enumerate(ex_q):
            gwq = lax.dynamic_update_slice(gwq, ex, ((1 - core) * CR, parts[n][0]))

        grad_w_qkv = jnp.transpose(gwq.reshape(3, NH, DH, D), (3, 0, 1, 2))
        grad_b_qkv = sums[3:6].reshape(3, NH, DH)
        return y_out, grad_x, sums[0], sums[1], grad_w_qkv, grad_b_qkv, gwo.reshape(NH, DH, D), sums[2]

    seq, rep = P(None, "sp", None), P()
    specs = (seq, seq) + (rep,) * 6
    return jax.shard_map(block, mesh=mesh, in_specs=specs, out_specs=specs, check_vma=False)
```

```python
import functools
import math

import jax
import jax.numpy as jnp
from jax import lax
from jax.experimental import pallas as pl
from jax.experimental.pallas import tpu as pltpu
from jax.sharding import PartitionSpec as P


LN_EPS = 1e-5
F32 = jnp.float32
BF16 = jnp.bfloat16
VMEM_LIMIT = 64 * 1024 * 1024 - 65536

B, S, D, NH, DH = 2, 2048, 3072, 32, 96
NDEV = 16
TOK = S // NDEV
GH = 4
GR = GH * DH
CR = 4 * GR
SCALE = DH ** -0.5
BQ = 512
LANES = 128


def dot_nt(a, b):
    return lax.dot_general(a, b, (((1,), (1,)), ((), ())), preferred_element_type=F32)


def dot_nn(a, b):
    return jnp.dot(a, b, preferred_element_type=F32)


def params(**kw):
    return pltpu.CompilerParams(vmem_limit_bytes=VMEM_LIMIT, **kw)


def cost(flops, moved):
    return pl.CostEstimate(flops=int(flops), bytes_accessed=int(moved), transcendentals=0)


ROWS = dict(axis=0, keepdims=True)
LAST_DIM = dict(axis=-1, keepdims=True)


def normalize(x):
    centered = x - jnp.mean(x, **LAST_DIM)
    inv_std = lax.rsqrt(jnp.mean(centered * centered, **LAST_DIM) + LN_EPS)
    return centered * inv_std, inv_std


def fixed(*shape):
    return pl.BlockSpec(shape, lambda *_: (0,) * len(shape))


def by_column(*shape):
    return pl.BlockSpec(shape, lambda j, *_: (0, j))


def aligned(start, size):
    return pl.ds(pl.multiple_of(start, size), size)


def run_all(copies, wait=False):
    for c in copies:
        c.wait() if wait else c.start()


dma = pltpu.SemaphoreType.DMA


def flip(index, bit):
    return index + bit * (1 - 2 * ((index // bit) % 2))


def att_head(q_ref, k_ref, v_ref, do_ref, o_ref, dq_ref, dk_ref, dv_ref, dk_acc, dv_acc):
    to_exp2 = SCALE * math.log2(math.e)
    k_t = k_ref[...]
    v_t = v_ref[...]
    k_n = k_t.T
    v_n = v_t.T
    db_q = jnp.zeros((DH, 1), F32)
    for i in reversed(range(S // BQ)):
        keys = (i + 1) * BQ
        cols = slice(i * BQ, keys)
        q = q_ref[:, cols]
        do = do_ref[:, cols]
        s = dot_nn(k_n[:keys], q)
        row = lax.broadcasted_iota(jnp.int32, (BQ, BQ), 0)
        col = lax.broadcasted_iota(jnp.int32, (BQ, BQ), 1)
        s_diag = jnp.where(row <= col, s[keys - BQ:], -1e30)
        s = jnp.concatenate([s[:keys - BQ], s_diag], axis=0) if i else s_diag
        m = jnp.max(s, **ROWS)
        p = jnp.exp2((s - m) * to_exp2)
        p = p * (1.0 / jnp.sum(p, **ROWS))
        p_low = p.astype(BF16)
        o = dot_nn(v_t[:, :keys], p_low)
        o_ref[:, cols] = o.astype(BF16)
        dp = dot_nn(v_n[:keys], do).astype(BF16).astype(F32)
        row_dot = jnp.sum(o * do.astype(F32), **ROWS)
        ds = (p * (dp - row_dot)).astype(BF16)
        dq = (dot_nn(k_t[:, :keys], ds) * SCALE).astype(BF16)
        dq_ref[:, cols] = dq
        db_q += jnp.sum(dq.astype(F32), **LAST_DIM)
        dk = dot_nt(q, ds)
        dv = dot_nt(do, p_low)
        if keys == S:
            dk_acc[...] = dk
            dv_acc[...] = dv
        else:
            dk_acc[:, :keys] += dk
            dv_acc[:, :keys] += dv
    dk = (dk_acc[...] * SCALE).astype(BF16)
    dv = dv_acc[...].astype(BF16)
    dk_ref[...] = dk
    dv_ref[...] = dv
    return db_q, jnp.sum(dk.astype(F32), **LAST_DIM), jnp.sum(dv.astype(F32), **LAST_DIM)


NEAR = (2, 4, 8)
VIA = {6: 4, 12: 8, 10: 2}
LAST = {12: 2, 10: 4, 6: 8}
SLOT = {d: i for i, d in enumerate((0, 2, 4, 8, 6, 12, 10, 14))}
N_SEND, N_RECV = 17, 9
GY, U = 1, 0
FAR = list(SLOT)[1:]
ATT = [(0, 0)] * GH
STEPS = [(b, 0) for b in range(B)] + [(0, d) for d in FAR] + ATT + [(1, d) for d in FAR] + ATT
AT0 = B + len(FAR)
AT1 = len(STEPS) - GH
NEXT1 = AT0 + GH
FETCH_HERE = (0, 2, 5, 8, NEXT1, 16, 17)
FETCH_NEXT = (0, 2, 3, 5, 6, NEXT1, 14, 17, 18)


def front_kernel(*refs):
    x_ref, gy_ref, gain_ref, lnb_ref, w_ref, wout_ref, b_ref = refs[:7]
    all_ref, *piece_refs = refs[7:12]
    far_refs = refs[12:15]
    db_ref = refs[15]
    (bias_ref, wt_ref, wo_ref, qkv_ref, do_ref, pair_ref, head_ref, u_ref, dk_acc, dv_acc,
     send_sem, recv_sem, peer_sem, own_sem, pair_sem, head_sem, w_sem, osend_sem, orecv_sem) = refs[16:]
    me = lax.axis_index("sp")
    near = {bit: flip(me, bit) for bit in NEAR}
    peer = flip(me, 1)
    src = {0: me, **near}
    src[6], src[12], src[10] = flip(near[2], 4), flip(near[4], 8), flip(near[8], 2)
    src[14] = flip(src[6], 8)
    chip = me // 2
    group = chip + (chip // 4) * (7 - 2 * chip)
    mine = 4 * (me % 2) + group
    third = D // 3
    mesh_id = pl.DeviceIdType.MESH
    sends = []

    def half(b, d, h):
        return all_ref.at[b, d, pl.ds(h * TOK, TOK)]

    def descriptor(b, h, n, kind, d):
        source = target = half(b, src[d if kind else 0], h)
        if kind == 0:
            source = own_rows(b, h)
            recv, to = recv_sem.at[b, h, SLOT[d] - 1], near[d]
        elif kind == 1:
            far = [e for e in VIA if VIA[e] == d][0]
            recv, to = recv_sem.at[b, h, SLOT[far] - 1], near[far - d]
        elif kind == 2:
            j = list(LAST).index(d)
            source = target = source.at[:, pl.ds(j * third, third)]
            recv, to = recv_sem.at[b, h, 6 + j], near[LAST[d]]
        else:
            if d == 0:
                source = own_rows(b, h)
            recv, to = peer_sem.at[b, h, SLOT[d]], peer
        return pltpu.make_async_remote_copy(
            src_ref=source, dst_ref=target, send_sem=send_sem.at[b, h, n], recv_sem=recv,
            device_id=(to,), device_id_type=mesh_id)

    def send(b, h, kind, d):
        spec = (b, h, sum(1 for other in sends if other[:2] == (b, h)), kind, d)
        sends.append(spec)
        descriptor(*spec).start()

    def arrived(target, sem):
        pltpu.make_async_copy(target, target, sem).wait()

    def own_rows(b, h):
        return gy_ref.at[b] if h == GY else half(b, me, U)

    def stage0(b, h):
        for bit in NEAR:
            send(b, h, 0, bit)

    def stage0_peer(b, h):
        send(b, h, 3, 0)

    def stage1(b, h):
        for d in NEAR:
            arrived(half(b, src[d], h), recv_sem.at[b, h, SLOT[d] - 1])
            send(b, h, 1, d)
            send(b, h, 3, d)

    def stage2(b, h):
        for d in LAST:
            arrived(half(b, src[d], h), recv_sem.at[b, h, SLOT[d] - 1])
            send(b, h, 2, d)
            send(b, h, 3, d)

    def stage3(b, h):
        for j in range(3):
            arrived(half(b, src[14], h).at[:, pl.ds(j * third, third)], recv_sem.at[b, h, 6 + j])
        send(b, h, 3, 14)

    def look_up(k, values):
        return sum(jnp.where(k == i, v, 0) for i, v in enumerate(values) if v)

    def pair_of(k):
        flips = look_up(k, [d // 2 for _, d in STEPS])
        x, y, z = (chip % 2 + flips) % 2, (chip // 2 + flips // 2) % 2, (chip // 4 + flips // 4) % 2
        return look_up(k, [b for b, _ in STEPS]), x + 2 * y + 4 * z, look_up(k, [SLOT[d] for _, d in STEPS])

    def fetch(k):
        b, source, slot = pair_of(k)
        for h in range(2):
            arrived(half(b, 2 * source, h), peer_sem.at[b, h, slot])
        pair_copy(k).start()

    def pair_copy(k):
        b, source, _ = pair_of(k)
        return pltpu.make_async_copy(all_ref.at[b, pl.ds(2 * source, 2)], pair_ref.at[k % 2], pair_sem.at[k % 2])

    def among(k, steps):
        return sum(jnp.where(k == i, 1, 0) for i in steps) > 0

    def project(k):
        @pl.when(among(k, FETCH_HERE))
        def _():
            fetch(k)

        pair_copy(k).wait()

        @pl.when(among(k, FETCH_NEXT))
        def _():
            fetch(k + 1)

        b, source, _ = pair_of(k)
        pair = pair_ref.at[k % 2]
        u = jnp.concatenate([pair[0, :TOK], pair[1, :TOK]], axis=0)
        gy = jnp.concatenate([pair[0, TOK:], pair[1, TOK:]], axis=0)
        cols = aligned(source * 2 * TOK, 2 * TOK)
        qkv_ref[b, :, cols] = (dot_nt(wt_ref[...], u) + bias_ref[...]).astype(BF16)
        do_ref[b, :, cols] = dot_nt(wo_ref[...], gy).astype(BF16)

    weights = [pltpu.make_async_copy(w_ref.at[t, mine], wt_ref.at[pl.ds(t * GR, GR)], w_sem.at[t]) for t in range(3)]
    weights.append(pltpu.make_async_copy(wout_ref.at[mine], wo_ref, w_sem.at[3]))
    for c in weights:
        c.start()

    barrier = pltpu.get_barrier_semaphore()
    for d in (peer, *near.values()):
        pl.semaphore_signal(barrier, inc=1, device_id=(d,), device_id_type=mesh_id)
    pl.semaphore_wait(barrier, 4)

    stage0(0, GY)
    for b in range(B):
        load = pltpu.make_async_copy(gy_ref.at[b], pair_ref.at[b, 0, pl.ds(TOK, TOK)], own_sem.at[3 * b])
        load.start()
        x = x_ref[b].astype(F32)
        u_ref[b] = (normalize(x)[0] * gain_ref[...] + lnb_ref[...]).astype(BF16)
        store = [pltpu.make_async_copy(u_ref.at[b], half(b, me, U), own_sem.at[3 * b + 1])]
        store[0].start()
        load.wait()
        store.append(pltpu.make_async_copy(pair_ref.at[b, 0, pl.ds(TOK, TOK)], half(b, me, GY), own_sem.at[3 * b + 2]))
        store[1].start()
        for c in store:
            c.wait()
        if b == 0:
            stage0(0, U)
        stage0_peer(b, U)
        stage0_peer(b, GY)
    on_diagonal = lax.broadcasted_iota(jnp.int32, (DH, DH), 0) == lax.broadcasted_iota(jnp.int32, (DH, DH), 1)
    for n in range(3 * GH):
        row = b_ref[n // GH, pl.ds(GH * mine + n % GH, 1), :]
        bias_ref[n * DH:(n + 1) * DH, :] = jnp.sum(jnp.where(on_diagonal, row, 0.0), **LAST_DIM)
    run_all(weights, True)

    def head_of(ref, i):
        return ref.at[aligned((i % GH) * DH, DH), aligned((i // GH) * S, S)]

    def local_copies(i):
        return [pltpu.make_async_copy(head_ref.at[i % 2, n], head_of(ref, i), head_sem.at[i % 2, n])
                for n, ref in enumerate(piece_refs)]

    def o_copies(i):
        return [pltpu.make_async_remote_copy(
            src_ref=head_of(piece_refs[0], i), dst_ref=head_of(far_refs[n], i), send_sem=osend_sem.at[i, n],
            recv_sem=orecv_sem.at[i, n], device_id=(near[bit],), device_id_type=mesh_id)
            for n, bit in enumerate(NEAR)]

    def stored(i):
        for c in local_copies(i):
            c.wait()

    def pass_on(i):
        for c in o_copies(i):
            c.start()

    def attend(i):
        b, h = i // GH, i % GH
        rows = lambda ref, t: ref.at[b, aligned(t * GR + h * DH, DH)]
        out = [head_ref.at[i % 2, n] for n in range(len(piece_refs))]
        sums = att_head(*(rows(qkv_ref, t) for t in range(3)), rows(do_ref, 0), *out, dk_acc, dv_acc)
        for t, db in enumerate(sums):
            db_ref[b, t, aligned(h * DH, DH), :] = jnp.broadcast_to(db, (DH, LANES))
        for c in local_copies(i):
            c.start()

        @pl.when(h > 0)
        def _():
            stored(i - 1)

        @pl.when(i > GH)
        def _():
            pass_on(i - 1)

    def first_o():
        stored(GH - 1)
        for i in range(GH):
            pass_on(i)

    duties = {
        2: [lambda: stage1(0, GY), lambda: stage1(0, U)],
        5: [lambda: stage2(0, GY), lambda: stage2(0, U), lambda: stage0(1, GY), lambda: stage0(1, U)],
        8: [lambda: stage3(0, GY), lambda: stage3(0, U)],
        AT0 + 1: [lambda: stage1(1, GY)],
        AT0 + 2: [lambda: stage1(1, U)],
        NEXT1: [lambda: stage2(1, GY)],
        15: [lambda: stage2(1, U), first_o],
        17: [lambda: stage3(1, GY), lambda: stage3(1, U)],
    }

    def step(k, carry):
        for at, calls in duties.items():
            @pl.when(k == at)
            def _():
                for call in calls:
                    call()

        attending = jnp.logical_or(jnp.logical_and(k >= AT0, k < NEXT1), k >= AT1)

        @pl.when(attending)
        def _():
            attend(k - jnp.where(k < NEXT1, AT0, AT1 - GH))

        @pl.when(jnp.logical_not(attending))
        def _():
            project(k)

        return carry

    lax.fori_loop(0, len(STEPS), step, 0)
    stored(B * GH - 1)
    pass_on(B * GH - 1)
    for spec in sends:
        descriptor(*spec).wait_send()
    for i in range(B * GH):
        for c in o_copies(i):
            c.wait()


def front(x_in, grad_y, gain, ln_bias, w_rows, w_out, bias):
    vmem = pl.BlockSpec(memory_space=pltpu.VMEM)
    anywhere = pl.BlockSpec(memory_space=pl.ANY)
    gathered = jax.ShapeDtypeStruct((B, NDEV, 2 * TOK, D), BF16)
    piece = jax.ShapeDtypeStruct((GR, B * S), BF16)
    return pl.pallas_call(
        front_kernel,
        in_specs=[vmem, anywhere, vmem, vmem, anywhere, anywhere, vmem],
        out_specs=[anywhere] * 8 + [vmem],
        out_shape=[gathered] + [piece] * 7 + [jax.ShapeDtypeStruct((B, 3, GR, LANES), F32)],
        scratch_shapes=[
            pltpu.VMEM((3 * GR, 1), F32),
            pltpu.VMEM((3 * GR, D), BF16),
            pltpu.VMEM((GR, D), BF16),
            pltpu.VMEM((B, 3 * GR, S), BF16),
            pltpu.VMEM((B, GR, S), BF16),
            pltpu.VMEM((2, 2, 2 * TOK, D), BF16),
            pltpu.VMEM((2, 4, DH, S), BF16),
            pltpu.VMEM((B, TOK, D), BF16),
            pltpu.VMEM((DH, S), F32),
            pltpu.VMEM((DH, S), F32),
            dma((B, 2, N_SEND)),
            dma((B, 2, N_RECV)),
            dma((B, 2, 8)),
            dma((6,)),
            dma((2,)),
            dma((2, 4)),
            dma((4,)),
            dma((B * GH, 3)),
            dma((B * GH, 3)),
        ],
        compiler_params=params(collective_id=0, has_side_effects=True),
        cost_estimate=cost(15e10, 2e8),
        name="front",
    )(x_in, grad_y, gain.reshape(1, D), ln_bias.reshape(1, D), w_rows, w_out.reshape(8, GR, D), bias)


def my_group(tbl, s):
    return aligned(tbl[3 + s] * GR, GR)


def collect_kernel(tbl, *refs):
    for s in range(4):
        for k in range(4):
            refs[-1][k * TOK:(k + 1) * TOK, my_group(tbl, s)] = refs[4 * k + s][...].T


def collect(tbl, pieces):
    spec = lambda k: pl.BlockSpec((GR, TOK), lambda i, t: (0, (k % B) * NDEV + t[1 + k // B]))
    return pl.pallas_call(
        collect_kernel,
        grid_spec=pltpu.PrefetchScalarGridSpec(
            num_scalar_prefetch=1, grid=(1,), in_specs=[spec(k) for k in range(4) for _ in pieces],
            out_specs=fixed(2 * B * TOK, CR)),
        out_shape=jax.ShapeDtypeStruct((2 * B * TOK, CR), BF16),
        compiler_params=params(),
        cost_estimate=cost(1e9, 3e6),
        name="collect",
    )(tbl, *pieces * 4)


BD = 256


def dw_kernel(t, n_in, parts, rows_at, puts, tbl, x0, x1, *refs):
    pieces = refs[:4]
    outs = refs[n_in:]
    buf_ref, *ex_refs = outs[:1 + len(parts)]
    lhs_ref, own_ref, sem, own_sem, ex_sem, put_sem = outs[-6:]
    j = pl.program_id(0)
    core = tbl[0]
    extra = list(refs[4:n_in])

    @pl.when(j == 0)
    def _():
        copies = [pltpu.make_async_copy(p, lhs_ref.at[my_group(tbl, s)], sem.at[s]) for s, p in enumerate(pieces)]
        run_all(copies)
        run_all(copies, True)

    def columns(step):
        return aligned(step * BD, BD)

    def own_out(step, wait=False):
        src = own_ref.at[step % 2]
        run_all([pltpu.make_async_copy(
            src, buf_ref.at[aligned((2 * t + core) * CR, CR), columns(step)], own_sem.at[step % 2])], wait)
        for (start, stop), ex_ref in zip(parts, ex_refs):
            @pl.when(jnp.logical_and(step * BD >= start, step * BD < stop))
            def _():
                cols = columns(step - start // BD)
                run_all([pltpu.make_async_copy(src, ex_ref.at[:, cols], ex_sem.at[step % 2])], wait)

    put_copies = []
    for n, (at, row_block) in enumerate(puts):
        rows = aligned((2 * row_block + 1 - core) * CR, CR)
        put_copies.append(pltpu.make_async_copy(extra.pop(0), outs[at].at[rows, columns(j)], put_sem.at[n]))
    run_all(put_copies)

    x = jnp.concatenate([ref[0, r] for ref in (x0, x1) for r in range(NDEV)], axis=0)
    res = dot_nn(lhs_ref[...], x)

    @pl.when(j >= 2)
    def _():
        own_out(j - 2, True)

    own_ref[j % 2] = res
    own_out(j)

    if rows_at is not None:
        @pl.when(j == 0)
        def _():
            for k in range(4):
                cols = aligned((k % B) * S + tbl[1 + k // B] * TOK, TOK)
                outs[rows_at][k * TOK:(k + 1) * TOK, :] = lhs_ref[:, cols].T

    run_all(put_copies, True)

    @pl.when(j == pl.num_programs(0) - 1)
    def _():
        own_out(j - 1, True)
        own_out(j, True)


def weight_grad(tbl, gathered, pieces, t, which, out_rows, prev=None, rows=True, puts=(), parts=((0, D),)):
    anywhere = pl.BlockSpec(memory_space=pl.ANY)
    x_spec = lambda b: pl.BlockSpec((1, NDEV, TOK, BD), lambda j, t: (b, 0, which, j))
    ins = [(x_spec(b), gathered) for b in range(B)] + [(anywhere, p) for p in pieces]
    outs = [(anywhere, (out_rows, D), F32)] + [(anywhere, (CR, stop - start), F32) for start, stop in parts]
    rows_at = None
    put_at = []
    if rows:
        rows_at = len(outs)
        outs.append((fixed(2 * B * TOK, CR), (2 * B * TOK, CR), BF16))
    ins += [(by_column(CR, BD), block) for block, *_ in puts]
    alias = {}
    if prev is not None:
        alias[1 + len(ins)] = 0
        ins.append((anywhere, prev))
    for _, row_block, buffer in puts:
        put_at.append((0 if buffer is None else len(outs), row_block))
        if buffer is not None:
            alias[1 + len(ins)] = len(outs)
            ins.append((anywhere, buffer))
            outs.append((anywhere, buffer.shape, F32))
    return pl.pallas_call(
        functools.partial(dw_kernel, t, len(ins) - B, parts, rows_at, put_at),
        grid_spec=pltpu.PrefetchScalarGridSpec(
            num_scalar_prefetch=1,
            grid=(D // BD,),
            in_specs=[spec for spec, _ in ins],
            out_specs=[spec for spec, *_ in outs],
            scratch_shapes=[
                pltpu.VMEM((CR, B * S), BF16),
                pltpu.VMEM((2, CR, BD), F32),
                dma((4,)), dma((2,)), dma((2,)), dma((2,)),
            ]),
        out_shape=[jax.ShapeDtypeStruct(*shape) for _, *shape in outs],
        input_output_aliases=alias,
        compiler_params=params(),
        cost_estimate=cost(2 * CR * D * B * S, 75e6),
        name="weight_grad",
    )(tbl, *(arg for _, arg in ins))


CB = 512


def contract_kernel(n, *refs):
    rows = jnp.concatenate([r[...] for r in refs[1:1 + n]], axis=1)
    weight = jnp.concatenate([r[...] for r in refs[1 + n:1 + 2 * n]], axis=0)
    acc = dot_nn(rows, weight)
    prev = refs[1 + 2 * n:-2]
    for k in range(2):
        part = acc[k * B * TOK:(k + 1) * B * TOK]
        refs[k - 2][...] = part + prev[k][...] if prev else part


def contract(tbl, rows, weight, blocks, prev=()):
    out = by_column(B * TOK, CB)
    w_spec = lambda block: pl.BlockSpec((CR, CB), lambda i, t: (2 * block + t[0], i))
    n = len(blocks)
    return pl.pallas_call(
        functools.partial(contract_kernel, n),
        grid_spec=pltpu.PrefetchScalarGridSpec(
            num_scalar_prefetch=1,
            grid=(D // CB,),
            in_specs=[fixed(2 * B * TOK, CR)] * n
            + [w_spec(block) for block in blocks] + [out] * len(prev),
            out_specs=[out] * 2),
        out_shape=[jax.ShapeDtypeStruct((B * TOK, D), F32)] * 2,
        compiler_params=params(),
        cost_estimate=cost(2 * B * TOK * D * D * n, 22e6),
        name="contract",
    )(tbl, *rows, *[weight] * n, *prev)


def finish_kernel(du_own, du_peer, x_ref, gy_ref, db_ref, gain_ref, gx_ref, sums_ref):
    x_hat, inv_std = normalize(x_ref[0].astype(F32))
    du = (du_own[...] + du_peer[...]).astype(BF16).astype(F32)
    gy = gy_ref[0].astype(F32)
    grad_hat = du * gain_ref[...]
    centered = grad_hat - jnp.mean(grad_hat, **LAST_DIM)
    gx_ref[0] = (gy + inv_std * (centered - x_hat * jnp.mean(grad_hat * x_hat, **LAST_DIM))).astype(BF16)

    @pl.when(pl.program_id(0) == 0)
    def _():
        sums_ref[...] = db_ref[...]

    for k, val in enumerate((du * x_hat, du, gy)):
        sums_ref[k:k + 1, :] += jnp.sum(val, **ROWS)


def finish_y_kernel(y_own, y_peer, x_ref, b_ref, y_ref):
    y_ref[0] = (x_ref[0].astype(F32) + (y_own[...] + y_peer[...] + b_ref[...])).astype(BF16)


def finish(kernel, partials, acts, vector, sums=None):
    more = [] if sums is None else [sums]
    act = pl.BlockSpec((1, TOK, D), lambda b: (b, 0, 0))
    grad = jax.ShapeDtypeStruct((B, TOK, D), BF16)
    return pl.pallas_call(
        kernel,
        grid=(B,),
        in_specs=[pl.BlockSpec((TOK, D), lambda b: (b, 0))] * len(partials) + [act] * len(acts)
        + [fixed(8, D) for _ in more] + [fixed(1, D)],
        out_specs=[act] + [fixed(8, D) for _ in more],
        out_shape=[grad] + [jax.ShapeDtypeStruct((8, D), F32) for _ in more],
        compiler_params=params(),
        cost_estimate=cost(1e8, 1e7),
        name="finish",
    )(*partials, *acts, *more, vector.reshape(1, D))


def solution(mesh):
    def permute(a, bit):
        return lax.ppermute(a, "sp", [(i, i ^ bit) for i in range(NDEV)])

    def block(x_in, grad_y, ln_gain, ln_bias, w_qkv, b_qkv, w_out, b_out):
        me = lax.axis_index("sp")
        core, chip = me % 2, me // 2
        group = lambda c: jnp.where(c < 4, c, 7 - c)
        groups = [group(chip ^ d) for d in (0, 1, 2, 4)]
        tbl = jnp.stack([core, me, me ^ 1] + groups).astype(jnp.int32)
        mine = 4 * core + groups[0]

        flat_w = jnp.transpose(w_qkv, (1, 2, 3, 0)).reshape(3 * D, D)
        gathered, o, dq, dk, dv, *far_o, db = front(
            x_in, grad_y, ln_gain, ln_bias, flat_w.reshape(3, 8, GR, D), w_out, b_qkv)

        pieces = {"o": [o] + far_o}
        for name, piece in (("v", dv), ("k", dk), ("q", dq)):
            pieces[name] = [piece] + [permute(piece, bit) for bit in NEAR]

        def swap(a):
            return permute(a, 1)

        def grad(name, *args, **kw):
            return weight_grad(tbl, gathered, pieces[name[0]], *args, **kw)

        def rows_times(*args):
            return contract(tbl, *args)

        gwo, ex_o, rows_o = grad("o", 0, GY, D)
        y_own, y_peer = rows_times([rows_o], w_out.reshape(D, D), [0])
        y_peer = swap(y_peer)
        ex_o = swap(ex_o)
        gwq, ex_v, rows_v = grad("v", 2, U, 3 * D)
        ex_v = swap(ex_v)
        du = rows_times([rows_v], flat_w, [2])
        gwq, ex_k, rows_k, gwo = grad("k", 1, U, 3 * D, gwq, puts=[(ex_o, 0, gwo)])
        ex_k = swap(ex_k)
        rows_q = collect(tbl, pieces["q"])
        du_own, du_peer = rows_times([rows_k, rows_q], flat_w, [1, 0], du)
        du_peer = swap(du_peer)
        parts = ((0, 2 * D // 3), (2 * D // 3, D))
        gwq, *ex_q = grad("q", 0, U, 3 * D, gwq, rows=False, puts=[(ex_v, 2, None), (ex_k, 1, None)], parts=parts)
        ex_q = [swap(ex) for ex in ex_q]
        y_out, = finish(finish_y_kernel, [y_own, y_peer], [x_in], b_out)
        db = jnp.where(chip < 4, db[0, :, :, 0] + db[1, :, :, 0], 0.0).reshape(3, 1, GR)
        sums = lax.dynamic_update_slice(jnp.zeros((8, 8, GR), F32), db, (3, mine, 0)).reshape(8, D)
        grad_x, sums = finish(finish_kernel, [du_own, du_peer], [x_in, grad_y], ln_gain, sums)
        for bit in (*NEAR, 1):
            sums = sums + permute(sums, bit)
        for n, ex in enumerate(ex_q):
            gwq = lax.dynamic_update_slice(gwq, ex, ((1 - core) * CR, parts[n][0]))

        grad_w_qkv = jnp.transpose(gwq.reshape(3, NH, DH, D), (3, 0, 1, 2))
        grad_b_qkv = sums[3:6].reshape(3, NH, DH)
        return y_out, grad_x, sums[0], sums[1], grad_w_qkv, grad_b_qkv, gwo.reshape(NH, DH, D), sums[2]

    seq, rep = P(None, "sp", None), P()
    specs = (seq, seq) + (rep,) * 6
    return jax.shard_map(block, mesh=mesh, in_specs=specs, out_specs=specs, check_vma=False)
```
